32 devices in a mesh: tp: 8 (over z, y), rep: 4 (over x, core).
Axes of the slice: x: 2, y: 2, z: 4, core: 2. Of those that a mesh axis runs over, the one named last changes fastest.
Arguments:
- tokens: bfloat16 [1536, 8192], P('rep', 'tp'), may hold values from -6 to 6
- row_lengths: int32 [8], P('rep'), may hold values from 1 to 192
- attn_gain: float32 [8192], P('tp'), may hold values from 0.1 to 1.9
- query_weight: bfloat16 [8192, 4096], P('rep', 'tp'), may hold values from -2 to 2
- key_weight: bfloat16 [8192, 512], P('rep', 'tp'), may hold values from -2 to 2
- value_matrix: bfloat16 [8192, 512], P('rep', 'tp'), may hold values from -0.0625 to 0.0625
- output_weight: bfloat16 [4096, 8192], P('rep', 'tp'), may hold values from -0.09375 to 0.09375
- final_gain: float32 [8192], P('tp'), may hold values from 0.1 to 1.9
- value_head: float32 [8192, 6], P('tp'), may hold values from -0.0625 to 0.0625
Outputs:
- resid_out: bfloat16 [1536, 8192], P('rep', 'tp')
- objective_scores: float32 [1536, 6], P('rep')
The draws below stay inside these ranges and needn't reach their ends.
All inputs are finite; a program needn't handle non-finite values.
Results may differ from the reference program's by a relative error of at most 0.025.
Values may be sent and summed in bfloat16 or wider, within the bound.
A program may use at most 64 MiB of HBM per device.

```python
import math
import jax
import jax.numpy as jnp
from jax import lax

MODEL_WIDTH = 8192
QUERY_HEADS = 32
KEY_VALUE_HEADS = 4
HEAD_SIZE = 128
NOBJ = 6
ROW_LENGTH = 192
TOKENS = 1536
SEQS = 8


def shared_keys(key):
    return jax.random.normal(jax.random.fold_in(key, 11), (MODEL_WIDTH, KEY_VALUE_HEADS * HEAD_SIZE), jnp.float32) / math.sqrt(MODEL_WIDTH)


def draw_key_weight(key, part):
    return jnp.clip(shared_keys(key), -2.0, 2.0).astype(jnp.bfloat16)


def draw_query_weight(key, part):
    noise = jax.random.normal(jax.random.fold_in(key, 23), (MODEL_WIDTH, QUERY_HEADS * HEAD_SIZE), jnp.float32) / math.sqrt(MODEL_WIDTH)
    return jnp.clip(noise, -2.0, 2.0).astype(jnp.bfloat16)


def set_ends(array, stream_key, least, high):
    longest = array.shape.index(max(array.shape))
    spots = []
    for shift in (0, 1):
        where = [jax.random.randint(jax.random.fold_in(stream_key, axis), (), 0, length) for axis, length in enumerate(array.shape)]
        where[longest] = (where[longest] + shift) % array.shape[longest]
        spots.append(tuple(where))
    return array.at[spots[0]].set(least).at[spots[1]].set(high)


def shard_levels(stream_key, dims, cuts, smallest, high):
    def one(dim, shards_of):
        draws = jax.random.uniform(jax.random.fold_in(jax.random.fold_in(stream_key, 6), dim), (shards_of,), jnp.float32, smallest / len(cuts), high / len(cuts))
        return jnp.repeat(jnp.exp(draws), dims[dim] // shards_of).reshape((-1,) + (1,) * (len(dims) - dim - 1))

    factor_of = one(*cuts[0])
    for cut in cuts[1:]:
        factor_of = factor_of * one(*cut)
    return factor_of


def normal_values(rng, dims, width, reach, split=(), held_as=jnp.bfloat16):
    level = shard_levels(rng, dims, split, -0.22, 0.18) if split else 1.0
    values = jax.random.normal(rng, dims, jnp.float32) * width * level
    return jnp.minimum(jnp.maximum(values, -reach), reach).astype(held_as)


def setup_inputs(seed: int = 0) -> dict:
    key_list = jax.random.split(jax.random.key(seed), 10)
    return {
        "tokens": normal_values(key_list[0], (TOKENS, MODEL_WIDTH), 1.0, 6.0, ((0, 4), (1, 8))),
        "row_lengths": set_ends(jax.random.randint(key_list[1], (SEQS,), 1, ROW_LENGTH + 1), jax.random.fold_in(key_list[1], 1), 1, ROW_LENGTH).astype(jnp.int32),
        "attn_gain": jnp.clip(1.0 + 0.18 * jax.random.normal(key_list[2], (MODEL_WIDTH,), jnp.float32), 0.1, 1.9),
        "query_weight": draw_query_weight(jax.random.fold_in(key_list[9], 71), 0),
        "key_weight": draw_key_weight(jax.random.fold_in(key_list[9], 71), 0),
        "value_matrix": normal_values(key_list[5], (MODEL_WIDTH, KEY_VALUE_HEADS * HEAD_SIZE), MODEL_WIDTH ** -0.5, 0.0625, ((0, 4), (1, 8))),
        "output_weight": normal_values(key_list[6], (QUERY_HEADS * HEAD_SIZE, MODEL_WIDTH), (QUERY_HEADS * HEAD_SIZE) ** -0.5, 0.09375, ((0, 4), (1, 8))),
        "final_gain": jnp.clip(1.0 + 0.18 * jax.random.normal(key_list[7], (MODEL_WIDTH,), jnp.float32), 0.1, 1.9),
        "value_head": normal_values(key_list[8], (MODEL_WIDTH, NOBJ), MODEL_WIDTH ** -0.5, 0.0625, ((0, 8),), jnp.float32),
    }


EPS = 1e-05

def reference(tokens, row_lengths, attn_gain, query_weight, key_weight, value_matrix, output_weight, final_gain, value_head):
    xf = tokens.astype(jnp.float32)
    first_scale = lax.rsqrt(lax.optimization_barrier(jnp.mean(xf * xf, axis=1, keepdims=True)) + EPS)
    normed = (xf * first_scale * attn_gain).astype(jnp.bfloat16)
    query = jnp.dot(normed, query_weight, preferred_element_type=jnp.float32).astype(jnp.bfloat16)
    key_rows = jnp.dot(normed, key_weight, preferred_element_type=jnp.float32).astype(jnp.bfloat16)
    value_rows = jnp.dot(normed, value_matrix, preferred_element_type=jnp.float32).astype(jnp.bfloat16)
    every_row = tokens.shape[0] // ROW_LENGTH
    query4 = query.reshape(every_row, ROW_LENGTH, QUERY_HEADS, HEAD_SIZE)
    key_tensor4 = key_rows.reshape(every_row, ROW_LENGTH, KEY_VALUE_HEADS, HEAD_SIZE)
    value_tensor4 = value_rows.reshape(every_row, ROW_LENGTH, KEY_VALUE_HEADS, HEAD_SIZE)
    position = jnp.arange(ROW_LENGTH, dtype=jnp.int32)
    causal = position[None, :] <= position[:, None]
    allowed = causal[None, :, :] & (position[None, None, :] < row_lengths[:, None, None])
    inv_root = 1.0 / HEAD_SIZE ** 0.5

    def one_head(index):
        qpart = lax.dynamic_index_in_dim(query4, index, 2, keepdims=False).astype(jnp.float32)
        shared = (index % KEY_VALUE_HEADS).astype(jnp.int32)
        kpart = lax.dynamic_index_in_dim(key_tensor4, shared, 2, keepdims=False).astype(jnp.float32)
        vpart = lax.dynamic_index_in_dim(value_tensor4, shared, 2, keepdims=False).astype(jnp.float32)
        scores = jnp.einsum('rqd,rkd->rqk', qpart, kpart) * inv_root
        scores = jnp.where(allowed, scores, jnp.float32(-1e+30))
        scores = scores - lax.optimization_barrier(jnp.max(scores, axis=2, keepdims=True))
        expo = jnp.exp(scores)
        probs = (expo / lax.optimization_barrier(jnp.sum(expo, axis=2, keepdims=True))).astype(jnp.bfloat16)
        probs = lax.optimization_barrier(probs).astype(jnp.float32)
        return jnp.einsum('rqk,rkd->rqd', probs, vpart).astype(jnp.bfloat16)
    heads = lax.map(one_head, jnp.arange(QUERY_HEADS, dtype=jnp.int32))
    attended = jnp.transpose(heads, (1, 2, 0, 3)).reshape(tokens.shape[0], QUERY_HEADS * HEAD_SIZE)
    update = jnp.dot(attended, output_weight, preferred_element_type=jnp.float32)
    resid_out = (xf + update).astype(jnp.bfloat16)
    rfloat = resid_out.astype(jnp.float32)
    final_scale = lax.rsqrt(lax.optimization_barrier(jnp.mean(rfloat * rfloat, axis=1, keepdims=True)) + EPS)
    weighted = jnp.dot(rfloat * final_gain, value_head, precision=lax.Precision.HIGHEST)
    logits = weighted * final_scale
    live = (position[None, :] < row_lengths[:, None]).reshape(tokens.shape[0], 1)
    objective_scores = jnp.where(live, logits, jnp.float32(0.0))
    return (resid_out, objective_scores)
```

```python
import functools
import jax
import jax.numpy as jnp
from jax import lax
from jax.experimental import pallas as pl
from jax.experimental.pallas import tpu as pltpu
from jax.sharding import PartitionSpec as P

KEY_VALUE_HEADS = 4
HEAD_SIZE = 128
EPS = 1e-05
MESH = pl.DeviceIdType.MESH
STEP = 256
SEMAPHORES = 512


class Stage:
    def __init__(self, src, dst, buffer, sems):
        self.into = pltpu.make_async_copy(src, buffer, sems.at[0])
        self.out = pltpu.make_async_copy(buffer, dst, sems.at[1])


def slot(ref, dim, size, index, rows=None):
    if rows is not None:
        return ref.at[pl.ds(*rows), pl.ds(pl.multiple_of(index * size, size), size)]
    if dim is None:
        return ref.at[index]
    if isinstance(dim, tuple):
        return ref.at[index, pl.ds(dim[2], dim[1])]
    start = pl.multiple_of(index * size, size)
    return ref.at[pl.ds(start, size)] if dim == 0 else ref.at[:, pl.ds(start, size)]


class Line:
    def __init__(self, axis, count, dim, src, dst, sems, rows=None):
        self.axis, self.dim, self.dst = axis, dim, dst
        self.windowed = isinstance(dim, tuple)
        rows = dim[:2] if self.windowed else rows
        self.src = src if rows is None else src.at[pl.ds(*rows)]
        self.rows = None if self.windowed else rows
        self.count = count
        self.up_sem, self.down_sem, self.pair_sem, self.line_recv, self.pair_recv = sems
        me = lax.axis_index(axis)
        self.me, self.place, self.side = me, me // 2, me % 2
        self.partner = me + 1 - 2 * self.side
        self.size = None if dim is None or self.windowed else src.shape[dim]

    def at(self, index):
        return slot(self.dst, self.dim, self.size, index, self.rows)

    def copy(self, source, index, send, recv, target):
        return pltpu.make_async_remote_copy(
            src_ref=source,
            dst_ref=self.at(index),
            send_sem=send,
            recv_sem=recv,
            device_id={self.axis: target},
            device_id_type=MESH,
        )

    def up(self, source, origin):
        return self.copy(
            source, 2 * origin + self.side, self.up_sem.at[origin], self.line_recv.at[origin], self.me + 2
        )

    def down(self, source, origin):
        return self.copy(
            source, 2 * origin + self.side, self.down_sem.at[origin], self.line_recv.at[origin], self.me - 2
        )

    def pair(self, source, origin):
        return self.copy(
            source,
            2 * origin + self.side,
            self.pair_sem.at[origin],
            self.pair_recv.at[origin],
            self.partner,
        )

    def own_block(self):
        return self.at(self.me)

    def has_up(self):
        return self.place < self.count - 1

    def has_down(self):
        return self.place > 0

    def begin(self):
        @pl.when(self.has_up())
        def _():
            self.up(self.src, self.place).start()

        @pl.when(self.has_down())
        def _():
            self.down(self.src, self.place).start()

        self.pair(self.src, self.place).start()

    def hop(self, step):
        below, above = self.place - step, self.place + step

        @pl.when(below >= 0)
        def _():
            block = self.at(2 * below + self.side)
            self.up(block, below).wait_recv()

            @pl.when(self.has_up())
            def _():
                self.up(block, below).start()

            self.pair(block, below).start()

        @pl.when(above < self.count)
        def _():
            block = self.at(2 * above + self.side)
            self.down(block, above).wait_recv()

            @pl.when(self.has_down())
            def _():
                self.down(block, above).start()

            self.pair(block, above).start()

    def finish(self):
        for origin in range(self.count):
            here = self.at(2 * origin + self.side)
            self.pair(here, origin).wait_send()
            pltpu.make_async_remote_copy(
                src_ref=here,
                dst_ref=self.at(2 * origin + 1 - self.side),
                send_sem=self.pair_sem.at[origin],
                recv_sem=self.pair_recv.at[origin],
                device_id={self.axis: self.partner},
                device_id_type=MESH,
            ).wait_recv()

            @pl.when((origin <= self.place) & self.has_up())
            def _():
                self.up(here, origin).wait_send()

            @pl.when((origin >= self.place) & self.has_down())
            def _():
                self.down(here, origin).wait_send()

    def neighbours(self):
        return ((self.has_up(), self.me + 2), (self.has_down(), self.me - 2), (None, self.partner))


class Cross(Line):
    def __init__(self, axis, count, dim, src, dst, sems, rows):
        super().__init__(axis, count, dim, src, dst, sems, rows)
        self.other = 1 - self.side

    def along(self, source, origin, side, which, step):
        sem = self.up_sem if step > 0 else self.down_sem
        return self.copy(
            source,
            2 * origin + side,
            sem.at[which * self.count + origin],
            self.line_recv.at[which * self.count + origin],
            self.me + step,
        )

    def spread(self, source, origin, which):
        side = self.side if which == 0 else self.other

        @pl.when(self.has_up() & (origin <= self.place))
        def _():
            self.along(source, origin, side, which, 2).start()

        @pl.when(self.has_down() & (origin >= self.place))
        def _():
            self.along(source, origin, side, which, -2).start()

    def across(self, index, source):
        return self.copy(source, index, self.pair_sem.at[0], self.pair_recv.at[0], self.partner)

    def begin(self):
        self.across(self.me, self.src).start()
        self.spread(self.src, self.place, 0)

    def turn(self):
        theirs = self.at(self.partner)
        self.across(self.partner, theirs).wait_recv()
        self.spread(theirs, self.place, 1)

    def hop(self, step):
        for which in range(2):
            side = self.side if which == 0 else self.other
            for origin in (self.place - step, self.place + step):

                @pl.when((origin >= 0) & (origin < self.count))
                def _(origin=origin, side=side, which=which):
                    block = self.at(2 * origin + side)
                    self.along(block, origin, side, which, 2).wait_recv()
                    self.spread(block, origin, which)

    def finish(self):
        self.across(self.me, self.src).wait_send()
        for which in range(2):
            side = self.side if which == 0 else self.other
            for origin in range(self.count):
                block = self.at(2 * origin + side)

                @pl.when((origin <= self.place) & self.has_up())
                def _(origin=origin, side=side, which=which, block=block):
                    self.along(block, origin, side, which, 2).wait_send()

                @pl.when((origin >= self.place) & self.has_down())
                def _(origin=origin, side=side, which=which, block=block):
                    self.along(block, origin, side, which, -2).wait_send()


class Direct:
    def __init__(self, axis, members, src, dst, sems):
        self.axis, self.members, self.src, self.dst = axis, members, src, dst
        self.send, self.recv = sems
        self.me = lax.axis_index(axis)

    def to(self, offset):
        return pltpu.make_async_remote_copy(
            src_ref=self.src,
            dst_ref=self.dst.at[self.me],
            send_sem=self.send.at[offset - 1],
            recv_sem=self.recv.at[offset - 1],
            device_id={self.axis: lax.rem(self.me + offset, self.members)},
            device_id_type=MESH,
        )

    def come(self, offset):
        return pltpu.make_async_remote_copy(
            src_ref=self.src,
            dst_ref=self.dst.at[lax.rem(self.me - offset + self.members, self.members)],
            send_sem=self.send.at[offset - 1],
            recv_sem=self.recv.at[offset - 1],
            device_id={self.axis: lax.rem(self.me + offset, self.members)},
            device_id_type=MESH,
        )

    def own_block(self):
        return self.dst.at[self.me]

    def begin(self):
        for offset in range(1, self.members):
            self.to(offset).start()

    def finish(self):
        for offset in range(1, self.members):
            self.to(offset).wait_send()
            self.come(offset).wait_recv()


def gather_kernel(plan, sizes, *refs):
    count = len(plan)
    sources, targets = refs[:count], refs[count : 2 * count]
    rest = list(refs[2 * count :])

    def take(number):
        taken = rest[:number]
        del rest[:number]
        return taken

    jobs, stages = [], []
    for (kind, axis, dim), src, dst in zip(plan, sources, targets):
        if kind == "fill":
            dst = targets[dim]
            buffer, sems = take(2)
            stages.append(Stage(src, dst.at[:, pl.ds(axis, src.shape[1])], buffer, sems))
            continue
        if kind == "direct":
            made = [Direct(axis, sizes[axis], src, dst, take(2))]
        elif kind == "line":
            made = [Line(axis, sizes[axis] // 2, dim, src, dst, take(5))]
        else:
            first, second = cut(src.shape[0])
            made = [
                Line(axis, sizes[axis] // 2, dim, src, dst, take(5), first),
                Cross(axis, sizes[axis] // 2, dim, src, dst, take(5), second),
            ]
        for job in made:
            buffer, sems = take(2)
            stages.append(Stage(job.src, job.own_block(), buffer, sems))
        jobs += made
    barrier = pltpu.get_barrier_semaphore()
    direct_axes = {job.axis for job in jobs if isinstance(job, Direct)}
    greeted, peers = set(), 0
    for job in jobs:
        if job.axis in greeted:
            continue
        greeted.add(job.axis)
        if job.axis in direct_axes:
            members = sizes[job.axis]
            peers = peers + members - 1
            for offset in range(1, members):
                pl.semaphore_signal(
                    barrier,
                    inc=1,
                    device_id={job.axis: lax.rem(job.me + offset, members)},
                    device_id_type=MESH,
                )
        else:
            for there, target in job.neighbours():
                def signal(target=target, job=job):
                    pl.semaphore_signal(
                        barrier, inc=1, device_id={job.axis: target}, device_id_type=MESH
                    )

                if there is None:
                    peers = peers + 1
                    signal()
                else:
                    peers = peers + there.astype(jnp.int32)
                    pl.when(there)(signal)
    pl.semaphore_wait(barrier, peers)
    for job in jobs:
        job.begin()
    for stage in stages:
        stage.into.start()
    for stage in stages:
        stage.into.wait()
        stage.out.start()
    for job in jobs:
        if isinstance(job, Cross):
            job.turn()
    for axis in ("tp", "rep"):
        lines = [job for job in jobs if isinstance(job, Line) and job.axis == axis]
        for step in range(1, max([job.count for job in lines], default=1)):
            for job in lines:
                job.hop(step)
    for job in jobs:
        job.finish()
    for stage in stages:
        stage.out.wait()


def cut(total):
    cross = total // (6 * 16) * 16
    return (0, total - cross), (total - cross, cross)


def gather(plan, sizes, arrays, collective_id, memory=pl.ANY):
    shapes, scratch = [], []
    dma = pltpu.SemaphoreType.DMA
    for (kind, axis, dim), array in zip(plan, arrays):
        if kind == "fill":
            shapes.append(jax.ShapeDtypeStruct((8, 128), array.dtype))
            scratch += [pltpu.VMEM(array.shape, array.dtype), dma((2,))]
            continue
        members = sizes[axis]
        if dim is None:
            shape = (members,) + array.shape
        elif isinstance(dim, tuple):
            shape = (members, dim[2] + dim[1]) + array.shape[1:]
        else:
            shape = tuple(n * members if i == dim else n for i, n in enumerate(array.shape))
        shapes.append(jax.ShapeDtypeStruct(shape, array.dtype))
        whole = pltpu.VMEM(array.shape, array.dtype)
        if kind == "direct":
            scratch += [dma((members - 1,))] * 2 + [whole, dma((2,))]
        elif kind == "line":
            if isinstance(dim, tuple):
                whole = pltpu.VMEM(dim[1:2] + array.shape[1:], array.dtype)
            scratch += [dma((members // 2,))] * 5 + [whole, dma((2,))]
        else:
            scratch += [dma((members // 2,))] * 5 + [dma((members,))] * 5
            for _, length in cut(array.shape[0]):
                scratch += [pltpu.VMEM((length,) + array.shape[1:], array.dtype), dma((2,))]
    return pl.pallas_call(
        functools.partial(gather_kernel, plan, sizes),
        out_shape=tuple(shapes),
        in_specs=[pl.BlockSpec(memory_space=memory)] * len(arrays),
        out_specs=tuple([pl.BlockSpec(memory_space=memory)] * len(arrays)),
        scratch_shapes=scratch,
        compiler_params=pltpu.CompilerParams(collective_id=collective_id, has_side_effects=True),
    )(*arrays)


def local(
    sizes,
    tokens,
    row_lengths,
    attn_gain,
    query_weight,
    key_weight,
    value_matrix,
    output_weight,
    final_gain,
    value_head,
):
    width = tokens.shape[1] * sizes["tp"]
    rows_here = tokens.shape[0]
    head_cols = query_weight.shape[1]
    kv_cols = key_weight.shape[1]
    xfloat = tokens.astype(jnp.float32)
    squares_here = jnp.sum(xfloat * xfloat, axis=1)[None, :]
    gained = (xfloat * attn_gain).astype(jnp.bfloat16)
    packed = jnp.concatenate([query_weight, key_weight, value_matrix], axis=1)
    first = output_weight.shape[0] // 16
    early = output_weight.shape[0] // 4
    columns, weights, out_first, squares_all = gather(
        (
            ("split", "tp", 1),
            ("line", "rep", 0),
            ("line", "rep", (0, first, 0)),
            ("direct", "tp", None),
        ),
        sizes,
        (gained, packed, output_weight, squares_here),
        0,
    )
    first_scale = lax.rsqrt(jnp.sum(squares_all, axis=(0, 1)) / width + EPS)[:, None]
    projected = jnp.dot(columns, weights, preferred_element_type=jnp.float32)
    projected = (projected * first_scale).astype(jnp.bfloat16)
    query = projected[:, :head_cols]
    kv_all, out_early = gather(
        (("line", "tp", None), ("line", "rep", (first, early, 0))),
        sizes,
        (projected[:, head_cols:], output_weight),
        1,
    )
    sequence_rows = row_lengths.shape[0]
    length = rows_here // sequence_rows
    local_heads = head_cols // HEAD_SIZE
    key_full = kv_all[:, :, :kv_cols].transpose(1, 0, 2).reshape(rows_here, -1)
    value_full = kv_all[:, :, kv_cols:].transpose(1, 0, 2).reshape(rows_here, -1)
    first_head = lax.axis_index("tp") * local_heads
    key_value_index = (first_head + jnp.arange(local_heads, dtype=jnp.int32)) % KEY_VALUE_HEADS
    query4 = query.reshape(sequence_rows, length, local_heads, HEAD_SIZE)
    key4 = key_full.reshape(sequence_rows, length, KEY_VALUE_HEADS, HEAD_SIZE)
    value4 = value_full.reshape(sequence_rows, length, KEY_VALUE_HEADS, HEAD_SIZE)
    if local_heads % KEY_VALUE_HEADS or local_heads != KEY_VALUE_HEADS:
        key4 = jnp.take(key4, key_value_index, axis=2)
        value4 = jnp.take(value4, key_value_index, axis=2)
    scores = jnp.einsum(
        "rqhd,rkhd->rhqk", query4, key4, preferred_element_type=jnp.float32
    ) * (1.0 / HEAD_SIZE**0.5)
    position = jnp.arange(length, dtype=jnp.int32)
    causal = position[None, :] <= position[:, None]
    allowed = causal[None, None, :, :] & (
        position[None, None, None, :] < row_lengths[:, None, None, None]
    )
    scores = jnp.where(allowed, scores, jnp.float32(-1e30))
    scores = scores - jnp.max(scores, axis=3, keepdims=True)
    expo = jnp.exp(scores)
    probs = (expo / jnp.sum(expo, axis=3, keepdims=True)).astype(jnp.bfloat16)
    attended = jnp.einsum(
        "rhqk,rkhd->rqhd", probs, value4, preferred_element_type=jnp.float32
    )
    attended = attended.astype(jnp.bfloat16).reshape(rows_here, head_cols)
    before = first + early
    late = (before, output_weight.shape[0] - before, before)
    mixed, out_weights, _, _ = gather(
        (("split", "tp", 1), ("line", "rep", late), ("fill", 0, 1), ("fill", first, 1)),
        sizes,
        (attended, output_weight, out_first, out_early),
        2,
    )
    out_weights = out_weights.reshape(-1, tokens.shape[1])
    update = jnp.dot(mixed, out_weights, preferred_element_type=jnp.float32)
    resid_out = (xfloat + update).astype(jnp.bfloat16)
    rfloat = resid_out.astype(jnp.float32)
    squares = jnp.sum(rfloat * rfloat, axis=1)
    local_scores = jnp.dot(rfloat * final_gain, value_head, precision=lax.Precision.HIGHEST)
    stats = jnp.concatenate([local_scores.T, squares[None, :]], axis=0)
    (stats_all,) = gather((("direct", "tp", None),), sizes, (stats,), 3)
    stats = jnp.sum(stats_all, axis=0)
    logits = (stats[:-1] * lax.rsqrt(stats[-1:] / width + EPS)).T
    live = (position[None, :] < row_lengths[:, None]).reshape(rows_here, 1)
    objective_scores = jnp.where(live, logits, jnp.float32(0.0))
    return (resid_out, objective_scores)


class Pool:
    def __init__(self, ref):
        self.ref, self.used = ref, 0

    def take(self, number):
        base = self.used
        self.used += number
        return lambda index: self.ref.at[base + index]


class Route:
    def __init__(self, axis, size, view, pool):
        self.axis, self.view, self.count = axis, view, size // 2
        self.me = lax.axis_index(axis)
        self.place, self.side = self.me // 2, self.me % 2
        self.partner = self.me + 1 - 2 * self.side
        self.has_up = self.place < self.count - 1
        self.has_down = self.place > 0
        self.pool = pool
        self.make(pool)

    def copy(self, index, send, recv, target):
        return pltpu.make_async_remote_copy(
            src_ref=self.view(index),
            dst_ref=self.view(index),
            send_sem=send,
            recv_sem=recv,
            device_id={self.axis: target},
            device_id_type=MESH,
        )


class Row(Route):
    def make(self, pool):
        n = self.count
        self.up_sem, self.down_sem, self.pair_sem = pool.take(n), pool.take(n), pool.take(n)
        self.line_recv, self.pair_recv = pool.take(n), pool.take(n)

    def up(self, origin):
        index = 2 * origin + self.side
        return self.copy(index, self.up_sem(origin), self.line_recv(origin), self.me + 2)

    def down(self, origin):
        index = 2 * origin + self.side
        return self.copy(index, self.down_sem(origin), self.line_recv(origin), self.me - 2)

    def pair(self, origin, side):
        index = 2 * origin + side
        return self.copy(index, self.pair_sem(origin), self.pair_recv(origin), self.partner)

    def begin(self):
        pl.when(self.has_up)(lambda: self.up(self.place).start())
        pl.when(self.has_down)(lambda: self.down(self.place).start())
        self.pair(self.place, self.side).start()

    def hop(self, step):
        below, above = self.place - step, self.place + step

        @pl.when(below >= 0)
        def _():
            self.up(below).wait_recv()
            pl.when(self.has_up)(lambda: self.up(below).start())
            self.pair(below, self.side).start()

        @pl.when(above < self.count)
        def _():
            self.down(above).wait_recv()
            pl.when(self.has_down)(lambda: self.down(above).start())
            self.pair(above, self.side).start()

    def gathered(self):
        for origin in range(self.count):
            self.pair(origin, 1 - self.side).wait_recv()

    def drain(self):
        for origin in range(self.count):
            self.pair(origin, self.side).wait_send()
            pl.when((origin <= self.place) & self.has_up)(lambda: self.up(origin).wait_send())
            pl.when((origin >= self.place) & self.has_down)(lambda: self.down(origin).wait_send())


class Crossed(Route):
    def make(self, pool):
        n = 2 * self.count
        self.up_sem, self.down_sem, self.line_recv = pool.take(n), pool.take(n), pool.take(n)
        self.pair_sem, self.pair_recv = pool.take(1), pool.take(1)
        self.sides = (self.side, 1 - self.side)

    def along(self, origin, which, step):
        number = which * self.count + origin
        sem = (self.up_sem if step > 0 else self.down_sem)(number)
        index = 2 * origin + self.sides[which]
        return self.copy(index, sem, self.line_recv(number), self.me + step)

    def spread(self, origin, which):
        up, down = self.has_up & (origin <= self.place), self.has_down & (origin >= self.place)
        pl.when(up)(lambda: self.along(origin, which, 2).start())
        pl.when(down)(lambda: self.along(origin, which, -2).start())

    def across(self, index):
        return self.copy(index, self.pair_sem(0), self.pair_recv(0), self.partner)

    def begin(self):
        self.across(self.me).start()
        self.spread(self.place, 0)

    def turn(self):
        self.across(self.partner).wait_recv()
        self.spread(self.place, 1)

    def hop(self, step):
        for which in range(2):
            for origin in (self.place - step, self.place + step):

                @pl.when((origin >= 0) & (origin < self.count))
                def _(origin=origin, which=which):
                    self.along(origin, which, 2).wait_recv()
                    self.spread(origin, which)

    def gathered(self):
        pass

    def drain(self):
        self.across(self.me).wait_send()
        for which in range(2):
            for origin in range(self.count):
                up = (origin <= self.place) & self.has_up
                down = (origin >= self.place) & self.has_down
                pl.when(up)(lambda: self.along(origin, which, 2).wait_send())
                pl.when(down)(lambda: self.along(origin, which, -2).wait_send())


class Both:
    def __init__(self, *parts):
        self.parts = parts

    def begin(self):
        for part in self.parts:
            part.begin()

    def turn(self):
        for part in self.parts:
            if isinstance(part, Crossed):
                part.turn()

    def hop(self, step):
        for part in self.parts:
            part.hop(step)

    def gathered(self):
        for part in self.parts:
            part.gathered()

    def drain(self):
        for part in self.parts:
            part.drain()


class Everyone:
    def __init__(self, axis, size, view, pool):
        self.axis, self.size, self.view = axis, size, view
        self.me = lax.axis_index(axis)
        self.send, self.recv = pool.take(size - 1), pool.take(size - 1)

    def copy(self, index, offset):
        return pltpu.make_async_remote_copy(
            src_ref=self.view(index),
            dst_ref=self.view(index),
            send_sem=self.send(offset - 1),
            recv_sem=self.recv(offset - 1),
            device_id={self.axis: lax.rem(self.me + offset, self.size)},
            device_id_type=MESH,
        )

    def begin(self):
        for offset in range(1, self.size):
            self.copy(self.me, offset).start()

    def gathered(self):
        for offset in range(1, self.size):
            self.copy(lax.rem(self.me - offset + self.size, self.size), offset).wait_recv()

    def drain(self):
        for offset in range(1, self.size):
            self.copy(self.me, offset).wait_send()


NT = (((1,), (1,)), ((), ()))


def dot(a, b):
    return jnp.dot(a, b, preferred_element_type=jnp.float32)


def dot_nt(a, b):
    return lax.dot_general(a, b, NT, preferred_element_type=jnp.float32)


def exact_parts(values, number):
    parts = []
    for _ in range(number):
        part = values.astype(jnp.bfloat16)
        parts.append(part)
        values = values - part.astype(jnp.float32)
    return parts


def row_sums_of_squares(block):
    wide = block.astype(jnp.float32)
    ones = jnp.ones((16, block.shape[1]), jnp.bfloat16)
    high, low = exact_parts(wide * wide, 2)
    return (dot_nt(ones, high) + dot_nt(ones, low))[:8]


def layer_kernel(
    sizes,
    lengths_s,
    tokens_h,
    gain_h,
    query_h,
    key_h,
    value_h,
    output_h,
    final_h,
    head_h,
    resid_h,
    score_h,
    tok_all,
    wkv_all,
    wq_all,
    wo_all,
    kv_all,
    att_all,
    sq_all,
    stat_all,
    raw,
    gain,
    fgain,
    heads,
    qbuf,
    resid,
    score,
    dma,
    local_dma,
):
    tp, rep = sizes["tp"], sizes["rep"]
    me_t, me_r = lax.axis_index("tp"), lax.axis_index("rep")
    pool, here = Pool(dma), Pool(local_dma)
    width = tp * tokens_h.shape[1]
    features = tokens_h.shape[1]
    sequences = lengths_s.shape[0]
    length = tokens_h.shape[0] // sequences
    kv_cols = key_h.shape[0]
    per_rep = tp // rep
    q_steps, q_cols = wq_all.shape[0], wq_all.shape[3]
    o_steps, o_cols = wo_all.shape[0], wo_all.shape[3]
    head_cols = q_steps * q_cols
    per_head = HEAD_SIZE // kv_cols
    crossing = length // (6 * 16) * 16

    def fetch(src, dst):
        made = pltpu.make_async_copy(src, dst, here.take(1)(0))
        made.start()
        return made

    def rows_of(s):
        return pl.ds(s * length, length)

    def gather_rows(buffer, s):
        start = s * length
        straight = pl.ds(start, length - crossing)
        rest = pl.ds(start + length - crossing, crossing)
        return Both(
            Crossed("tp", tp, lambda i: buffer.at[i, rest], pool),
            Row("tp", tp, lambda i: buffer.at[i, straight], pool),
        )

    token_jobs = [gather_rows(tok_all, s) for s in range(sequences)]
    att_jobs = [gather_rows(att_all, s) for s in range(sequences)]
    kv_jobs = [Row("tp", tp, lambda i, s=s: kv_all.at[s, i], pool) for s in range(sequences)]
    wkv_job = Row("rep", rep, lambda i: wkv_all.at[i], pool)
    wq_jobs = [Row("rep", rep, lambda i, j=j: wq_all.at[j, i], pool) for j in range(q_steps)]
    wo_jobs = [Row("rep", rep, lambda i, n=n: wo_all.at[n, i], pool) for n in range(o_steps)]
    sq_job = Everyone("tp", tp, lambda i: sq_all.at[i], pool)
    stat_jobs = [Everyone("tp", tp, lambda i, s=s: stat_all.at[s, i], pool) for s in range(sequences)]

    load_tokens = fetch(tokens_h, raw)
    load_gain = fetch(gain_h, gain)
    load_kv = [
        fetch(key_h, wkv_all.at[me_r, pl.ds(0, kv_cols)]),
        fetch(value_h, wkv_all.at[me_r, pl.ds(kv_cols, kv_cols)]),
    ]
    load_q = [
        fetch(query_h.at[:, pl.ds(j * q_cols, q_cols)], wq_all.at[j, me_r]) for j in range(q_steps)
    ]
    load_o = [
        fetch(output_h.at[:, pl.ds(n * o_cols, o_cols)], wo_all.at[n, me_r]) for n in range(o_steps)
    ]
    load_final = [fetch(final_h, fgain), fetch(head_h, heads)]

    barrier = pltpu.get_barrier_semaphore()
    for axis, me, size in (("tp", me_t, tp), ("rep", me_r, rep)):
        for offset in range(1, size):
            pl.semaphore_signal(
                barrier,
                inc=1,
                device_id={axis: lax.rem(me + offset, size)},
                device_id_type=MESH,
            )

    load_tokens.wait()
    load_gain.wait()
    for s in range(sequences):
        block = raw[rows_of(s), :].astype(jnp.float32) * gain[...]
        tok_all[me_t, rows_of(s), :] = block.astype(jnp.bfloat16)
    for copy in load_kv:
        copy.wait()
    pl.semaphore_wait(barrier, tp + rep - 2)

    token_jobs[0].begin()
    wkv_job.begin()
    for copy, job in zip(load_q, wq_jobs):
        copy.wait()
        job.begin()
    for copy, job in zip(load_o, wo_jobs):
        copy.wait()
        job.begin()
    sq_all[me_t] = row_sums_of_squares(raw[...])
    token_jobs[0].turn()
    sq_job.begin()
    for copy in load_final:
        copy.wait()
    token_jobs[0].hop(1)
    for job in token_jobs[1:]:
        job.begin()
        job.turn()
    wkv_job.hop(1)
    for step in range(2, rep // 2):
        wkv_job.hop(step)

    def row_scale(s):
        total = sq_all[0, :, rows_of(s)]
        for t in range(1, tp):
            total = total + sq_all[t, :, rows_of(s)]
        return lax.rsqrt(total / width + EPS)

    def project_kv(s):
        total = jnp.zeros((2 * kv_cols, length), jnp.float32)
        for t in range(tp):
            weight = wkv_all[t // per_rep, :, pl.ds(t % per_rep * features, features)]
            total = total + dot_nt(weight, tok_all[t, rows_of(s), :])
        kv_all[s, me_t] = (total * row_scale(s)[:1]).astype(jnp.bfloat16)
        kv_jobs[s].begin()

    def project_q(s, j):
        total = jnp.zeros((length, q_cols), jnp.float32)
        for t in range(tp):
            weight = wq_all[j, t // per_rep, pl.ds(t % per_rep * features, features), :]
            total = total + dot(tok_all[t, rows_of(s), :], weight)
        column = row_scale(s).T[:, :1]
        qbuf[s, :, pl.ds(j * q_cols, q_cols)] = (total * column).astype(jnp.bfloat16)

    def attend(s):
        here_length = lengths_s[s]
        query_at = lax.broadcasted_iota(jnp.int32, (length, length), 0)
        key_at = lax.broadcasted_iota(jnp.int32, (length, length), 1)
        allowed = (key_at <= query_at) & (key_at < here_length)
        for h in range(head_cols // HEAD_SIZE):
            first = h % KEY_VALUE_HEADS * per_head
            blocks = [kv_all[s, first + b] for b in range(per_head)]
            keys = jnp.concatenate([b[:kv_cols] for b in blocks], axis=0)
            values = jnp.concatenate([b[kv_cols:] for b in blocks], axis=0)
            query = qbuf[s, :, pl.ds(h * HEAD_SIZE, HEAD_SIZE)]
            scores = dot(query, keys) * (1.0 / HEAD_SIZE**0.5)
            scores = jnp.where(allowed, scores, jnp.float32(-1e30))
            expo = jnp.exp(scores - jnp.max(scores, axis=1, keepdims=True))
            probs = (expo / jnp.sum(expo, axis=1, keepdims=True)).astype(jnp.bfloat16)
            mixed = dot_nt(probs, values).astype(jnp.bfloat16)
            att_all[me_t, rows_of(s), pl.ds(h * HEAD_SIZE, HEAD_SIZE)] = mixed
        att_jobs[s].begin()

    def project_out(s, n):
        cols = pl.ds(n * o_cols, o_cols)
        total = raw[rows_of(s), cols].astype(jnp.float32)
        update = jnp.zeros((length, o_cols), jnp.float32)
        for t in range(tp):
            weight = wo_all[n, t // per_rep, pl.ds(t % per_rep * head_cols, head_cols), :]
            update = update + dot(att_all[t, rows_of(s), :], weight)
        resid[rows_of(s), cols] = (total + update).astype(jnp.bfloat16)

    def statistics(s):
        block = resid[rows_of(s), :]
        weight = heads[...] * fgain[...]
        weight = jnp.concatenate([weight, jnp.zeros((8 - heads.shape[0], features), jnp.float32)], axis=0)
        parts = [p.astype(jnp.float32) for p in exact_parts(weight, 3)]
        stacked = jnp.concatenate(parts + [jnp.zeros_like(weight)], axis=0).astype(jnp.bfloat16)
        sums = dot_nt(stacked, block)
        sums = sums[0:8] + sums[8:16] + sums[16:24]
        squares = row_sums_of_squares(block)
        line = lax.broadcasted_iota(jnp.int32, sums.shape, 0)
        stat_all[s, me_t] = jnp.where(line == 7, squares, sums)
        stat_jobs[s].begin()

    def conclude(s):
        stat_jobs[s].gathered()
        total = stat_all[s, 0]
        for t in range(1, tp):
            total = total + stat_all[s, t]
        score[s] = total * lax.rsqrt(total[7:8] / width + EPS)

    def write_out(s):
        return fetch(resid.at[rows_of(s)], resid_h.at[rows_of(s)])

    token_jobs[0].hop(2)
    token_jobs[1].hop(1)
    for step in range(3, tp // 2):
        token_jobs[0].hop(step)
        token_jobs[1].hop(step - 1)
    wq_jobs[0].hop(1)
    token_jobs[0].gathered()
    sq_job.gathered()
    wkv_job.gathered()
    project_kv(0)
    token_jobs[1].hop(tp // 2 - 1)
    wq_jobs[0].gathered()
    project_q(0, 0)
    for step in range(1, tp // 2):
        kv_jobs[0].hop(step)
    for j in range(1, q_steps):
        wq_jobs[j].hop(1)
        wq_jobs[j].gathered()
        project_q(0, j)
    kv_jobs[0].gathered()
    attend(0)
    token_jobs[1].gathered()
    project_kv(1)
    att_jobs[0].turn()
    kv_jobs[1].hop(1)
    project_q(1, 0)
    att_jobs[0].hop(1)
    kv_jobs[1].hop(2)
    for j in range(1, q_steps):
        project_q(1, j)
    for step in range(3, tp // 2):
        kv_jobs[1].hop(step)
    kv_jobs[1].gathered()
    attend(1)
    wo_jobs[0].hop(1)
    att_jobs[1].turn()
    att_jobs[0].hop(2)
    wo_jobs[1].hop(1)
    att_jobs[1].hop(1)
    for step in range(3, tp // 2):
        att_jobs[0].hop(step)
        att_jobs[1].hop(step - 1)
    att_jobs[0].gathered()
    for n in range(2):
        wo_jobs[n].gathered()
        project_out(0, n)
    att_jobs[1].hop(tp // 2 - 1)
    for n in range(2, o_steps):
        wo_jobs[n].hop(1)
        wo_jobs[n].gathered()
        project_out(0, n)
    statistics(0)
    writes = [write_out(0)]
    att_jobs[1].gathered()
    for n in range(o_steps):
        project_out(1, n)
    statistics(1)
    writes.append(write_out(1))
    conclude(0)
    conclude(1)
    last = fetch(score, score_h)
    for job in token_jobs + att_jobs + kv_jobs + [wkv_job] + wq_jobs + wo_jobs + [sq_job] + stat_jobs:
        job.drain()
    for copy in writes:
        copy.wait()
    last.wait()


def whole_layer(
    sizes,
    tokens,
    row_lengths,
    attn_gain,
    query_weight,
    key_weight,
    value_matrix,
    output_weight,
    final_gain,
    value_head,
):
    tp, rep = sizes["tp"], sizes["rep"]
    rows, features = tokens.shape
    sequences = row_lengths.shape[0]
    length = rows // sequences
    depth, head_cols = query_weight.shape
    kv_cols = key_weight.shape[1]
    mixed = output_weight.shape[0]
    vmem, dma = pltpu.VMEM, pltpu.SemaphoreType.DMA
    half, single = jnp.bfloat16, jnp.float32
    q_steps, o_steps = head_cols // STEP, features // STEP
    anywhere = pl.BlockSpec(memory_space=pl.ANY)
    resid, score = pl.pallas_call(
        functools.partial(layer_kernel, sizes),
        out_shape=(
            jax.ShapeDtypeStruct((rows, features), half),
            jax.ShapeDtypeStruct((sequences, 8, length), single),
        ),
        in_specs=[pl.BlockSpec(memory_space=pltpu.SMEM)] + [anywhere] * 8,
        out_specs=(anywhere, anywhere),
        scratch_shapes=[
            vmem((tp, rows, features), half),
            vmem((rep, 2 * kv_cols, depth), half),
            vmem((q_steps, rep, depth, STEP), half),
            vmem((o_steps, rep, mixed, STEP), half),
            vmem((sequences, tp, 2 * kv_cols, length), half),
            vmem((tp, rows, head_cols), half),
            vmem((tp, 8, rows), single),
            vmem((sequences, tp, 8, length), single),
            vmem((rows, features), half),
            vmem((1, features), single),
            vmem((1, features), single),
            vmem((value_head.shape[1], features), single),
            vmem((sequences, length, head_cols), half),
            vmem((rows, features), half),
            vmem((sequences, 8, length), single),
            dma((SEMAPHORES,)),
            dma((32,)),
        ],
        compiler_params=pltpu.CompilerParams(
            collective_id=4, has_side_effects=True, vmem_limit_bytes=64 * 1024 * 1024 - 128 * 1024
        ),
    )(
        row_lengths,
        tokens,
        attn_gain[None, :],
        query_weight,
        key_weight.T,
        value_matrix.T,
        output_weight,
        final_gain[None, :],
        value_head.T,
    )
    position = jnp.arange(length, dtype=jnp.int32)
    live = position[None, :] < row_lengths[:, None]
    score = jnp.where(live[:, None, :], score[:, : value_head.shape[1]], jnp.float32(0.0))
    return resid, score.transpose(0, 2, 1).reshape(rows, -1)


def fits(sizes, tokens, row_lengths, query_weight, key_weight):
    heads = query_weight.shape[1] // HEAD_SIZE
    return (
        row_lengths.shape[0] == 2
        and sizes["rep"] == 4
        and sizes["tp"] % sizes["rep"] == 0
        and sizes["tp"] >= 8
        and heads > 0
        and heads % KEY_VALUE_HEADS == 0
        and query_weight.shape[1] % STEP == 0
        and tokens.shape[1] % STEP == 0
        and HEAD_SIZE % key_weight.shape[1] == 0
    )


def layer(sizes, tokens, row_lengths, attn_gain, query_weight, key_weight, *rest):
    chosen = whole_layer if fits(sizes, tokens, row_lengths, query_weight, key_weight) else local
    return chosen(sizes, tokens, row_lengths, attn_gain, query_weight, key_weight, *rest)


def solution(mesh):
    in_specs = (
        P("rep", "tp"),
        P("rep"),
        P("tp"),
        P("rep", "tp"),
        P("rep", "tp"),
        P("rep", "tp"),
        P("rep", "tp"),
        P("tp"),
        P("tp", None),
    )
    out_specs = (P("rep", "tp"), P("rep", None))
    body = functools.partial(layer, dict(mesh.shape))
    return jax.shard_map(body, mesh=mesh, in_specs=in_specs, out_specs=out_specs, check_vma=False)
```

```python
import functools
import jax
import jax.numpy as jnp
from jax import lax
from jax.experimental import pallas as pl
from jax.experimental.pallas import tpu as pltpu
from jax.sharding import PartitionSpec as P

KEY_VALUE_HEADS = 4
HEAD_SIZE = 128
EPS = 1e-05
MESH = pl.DeviceIdType.MESH
STEP = 256
SEMAPHORES = 126


class Stage:
    def __init__(self, src, dst, buffer, sems):
        self.into = pltpu.make_async_copy(src, buffer, sems.at[0])
        self.out = pltpu.make_async_copy(buffer, dst, sems.at[1])


def slot(ref, dim, size, index, rows=None):
    if rows is not None:
        return ref.at[pl.ds(*rows), pl.ds(pl.multiple_of(index * size, size), size)]
    if dim is None:
        return ref.at[index]
    if isinstance(dim, tuple):
        return ref.at[index, pl.ds(dim[2], dim[1])]
    start = pl.multiple_of(index * size, size)
    return ref.at[pl.ds(start, size)] if dim == 0 else ref.at[:, pl.ds(start, size)]


class Line:
    def __init__(self, axis, count, dim, src, dst, sems, rows=None):
        self.axis, self.dim, self.dst = axis, dim, dst
        self.windowed = isinstance(dim, tuple)
        rows = dim[:2] if self.windowed else rows
        self.src = src if rows is None else src.at[pl.ds(*rows)]
        self.rows = None if self.windowed else rows
        self.count = count
        self.up_sem, self.down_sem, self.pair_sem, self.line_recv, self.pair_recv = sems
        me = lax.axis_index(axis)
        self.me, self.place, self.side = me, me // 2, me % 2
        self.partner = me + 1 - 2 * self.side
        self.size = None if dim is None or self.windowed else src.shape[dim]

    def at(self, index):
        return slot(self.dst, self.dim, self.size, index, self.rows)

    def copy(self, source, index, send, recv, target):
        return pltpu.make_async_remote_copy(
            src_ref=source,
            dst_ref=self.at(index),
            send_sem=send,
            recv_sem=recv,
            device_id={self.axis: target},
            device_id_type=MESH,
        )

    def up(self, source, origin):
        return self.copy(
            source, 2 * origin + self.side, self.up_sem.at[origin], self.line_recv.at[origin], self.me + 2
        )

    def down(self, source, origin):
        return self.copy(
            source, 2 * origin + self.side, self.down_sem.at[origin], self.line_recv.at[origin], self.me - 2
        )

    def pair(self, source, origin):
        return self.copy(
            source,
            2 * origin + self.side,
            self.pair_sem.at[origin],
            self.pair_recv.at[origin],
            self.partner,
        )

    def own_block(self):
        return self.at(self.me)

    def has_up(self):
        return self.place < self.count - 1

    def has_down(self):
        return self.place > 0

    def begin(self):
        @pl.when(self.has_up())
        def _():
            self.up(self.src, self.place).start()

        @pl.when(self.has_down())
        def _():
            self.down(self.src, self.place).start()

        self.pair(self.src, self.place).start()

    def hop(self, step):
        below, above = self.place - step, self.place + step

        @pl.when(below >= 0)
        def _():
            block = self.at(2 * below + self.side)
            self.up(block, below).wait_recv()

            @pl.when(self.has_up())
            def _():
                self.up(block, below).start()

            self.pair(block, below).start()

        @pl.when(above < self.count)
        def _():
            block = self.at(2 * above + self.side)
            self.down(block, above).wait_recv()

            @pl.when(self.has_down())
            def _():
                self.down(block, above).start()

            self.pair(block, above).start()

    def finish(self):
        for origin in range(self.count):
            here = self.at(2 * origin + self.side)
            self.pair(here, origin).wait_send()
            pltpu.make_async_remote_copy(
                src_ref=here,
                dst_ref=self.at(2 * origin + 1 - self.side),
                send_sem=self.pair_sem.at[origin],
                recv_sem=self.pair_recv.at[origin],
                device_id={self.axis: self.partner},
                device_id_type=MESH,
            ).wait_recv()

            @pl.when((origin <= self.place) & self.has_up())
            def _():
                self.up(here, origin).wait_send()

            @pl.when((origin >= self.place) & self.has_down())
            def _():
                self.down(here, origin).wait_send()

    def neighbours(self):
        return ((self.has_up(), self.me + 2), (self.has_down(), self.me - 2), (None, self.partner))


class Cross(Line):
    def __init__(self, axis, count, dim, src, dst, sems, rows):
        super().__init__(axis, count, dim, src, dst, sems, rows)
        self.other = 1 - self.side

    def along(self, source, origin, side, which, step):
        sem = self.up_sem if step > 0 else self.down_sem
        return self.copy(
            source,
            2 * origin + side,
            sem.at[which * self.count + origin],
            self.line_recv.at[which * self.count + origin],
            self.me + step,
        )

    def spread(self, source, origin, which):
        side = self.side if which == 0 else self.other

        @pl.when(self.has_up() & (origin <= self.place))
        def _():
            self.along(source, origin, side, which, 2).start()

        @pl.when(self.has_down() & (origin >= self.place))
        def _():
            self.along(source, origin, side, which, -2).start()

    def across(self, index, source):
        return self.copy(source, index, self.pair_sem.at[0], self.pair_recv.at[0], self.partner)

    def begin(self):
        self.across(self.me, self.src).start()
        self.spread(self.src, self.place, 0)

    def turn(self):
        theirs = self.at(self.partner)
        self.across(self.partner, theirs).wait_recv()
        self.spread(theirs, self.place, 1)

    def hop(self, step):
        for which in range(2):
            side = self.side if which == 0 else self.other
            for origin in (self.place - step, self.place + step):

                @pl.when((origin >= 0) & (origin < self.count))
                def _(origin=origin, side=side, which=which):
                    block = self.at(2 * origin + side)
                    self.along(block, origin, side, which, 2).wait_recv()
                    self.spread(block, origin, which)

    def finish(self):
        self.across(self.me, self.src).wait_send()
        for which in range(2):
            side = self.side if which == 0 else self.other
            for origin in range(self.count):
                block = self.at(2 * origin + side)

                @pl.when((origin <= self.place) & self.has_up())
                def _(origin=origin, side=side, which=which, block=block):
                    self.along(block, origin, side, which, 2).wait_send()

                @pl.when((origin >= self.place) & self.has_down())
                def _(origin=origin, side=side, which=which, block=block):
                    self.along(block, origin, side, which, -2).wait_send()


class Direct:
    def __init__(self, axis, members, src, dst, sems):
        self.axis, self.members, self.src, self.dst = axis, members, src, dst
        self.send, self.recv = sems
        self.me = lax.axis_index(axis)

    def to(self, offset):
        return pltpu.make_async_remote_copy(
            src_ref=self.src,
            dst_ref=self.dst.at[self.me],
            send_sem=self.send.at[offset - 1],
            recv_sem=self.recv.at[offset - 1],
            device_id={self.axis: lax.rem(self.me + offset, self.members)},
            device_id_type=MESH,
        )

    def come(self, offset):
        return pltpu.make_async_remote_copy(
            src_ref=self.src,
            dst_ref=self.dst.at[lax.rem(self.me - offset + self.members, self.members)],
            send_sem=self.send.at[offset - 1],
            recv_sem=self.recv.at[offset - 1],
            device_id={self.axis: lax.rem(self.me + offset, self.members)},
            device_id_type=MESH,
        )

    def own_block(self):
        return self.dst.at[self.me]

    def begin(self):
        for offset in range(1, self.members):
            self.to(offset).start()

    def finish(self):
        for offset in range(1, self.members):
            self.to(offset).wait_send()
            self.come(offset).wait_recv()


def gather_kernel(plan, sizes, *refs):
    count = len(plan)
    sources, targets = refs[:count], refs[count : 2 * count]
    rest = list(refs[2 * count :])

    def take(number):
        taken = rest[:number]
        del rest[:number]
        return taken

    jobs, stages = [], []
    for (kind, axis, dim), src, dst in zip(plan, sources, targets):
        if kind == "fill":
            dst = targets[dim]
            buffer, sems = take(2)
            stages.append(Stage(src, dst.at[:, pl.ds(axis, src.shape[1])], buffer, sems))
            continue
        if kind == "direct":
            made = [Direct(axis, sizes[axis], src, dst, take(2))]
        elif kind == "line":
            made = [Line(axis, sizes[axis] // 2, dim, src, dst, take(5))]
        else:
            first, second = cut(src.shape[0])
            made = [
                Line(axis, sizes[axis] // 2, dim, src, dst, take(5), first),
                Cross(axis, sizes[axis] // 2, dim, src, dst, take(5), second),
            ]
        for job in made:
            buffer, sems = take(2)
            stages.append(Stage(job.src, job.own_block(), buffer, sems))
        jobs += made
    barrier = pltpu.get_barrier_semaphore()
    direct_axes = {job.axis for job in jobs if isinstance(job, Direct)}
    greeted, peers = set(), 0
    for job in jobs:
        if job.axis in greeted:
            continue
        greeted.add(job.axis)
        if job.axis in direct_axes:
            members = sizes[job.axis]
            peers = peers + members - 1
            for offset in range(1, members):
                pl.semaphore_signal(
                    barrier,
                    inc=1,
                    device_id={job.axis: lax.rem(job.me + offset, members)},
                    device_id_type=MESH,
                )
        else:
            for there, target in job.neighbours():
                def signal(target=target, job=job):
                    pl.semaphore_signal(
                        barrier, inc=1, device_id={job.axis: target}, device_id_type=MESH
                    )

                if there is None:
                    peers = peers + 1
                    signal()
                else:
                    peers = peers + there.astype(jnp.int32)
                    pl.when(there)(signal)
    pl.semaphore_wait(barrier, peers)
    for job in jobs:
        job.begin()
    for stage in stages:
        stage.into.start()
    for stage in stages:
        stage.into.wait()
        stage.out.start()
    for job in jobs:
        if isinstance(job, Cross):
            job.turn()
    for axis in ("tp", "rep"):
        lines = [job for job in jobs if isinstance(job, Line) and job.axis == axis]
        for step in range(1, max([job.count for job in lines], default=1)):
            for job in lines:
                job.hop(step)
    for job in jobs:
        job.finish()
    for stage in stages:
        stage.out.wait()


def cut(total):
    cross = total // (6 * 16) * 16
    return (0, total - cross), (total - cross, cross)


def gather(plan, sizes, arrays, collective_id, memory=pl.ANY):
    shapes, scratch = [], []
    dma = pltpu.SemaphoreType.DMA
    for (kind, axis, dim), array in zip(plan, arrays):
        if kind == "fill":
            shapes.append(jax.ShapeDtypeStruct((8, 128), array.dtype))
            scratch += [pltpu.VMEM(array.shape, array.dtype), dma((2,))]
            continue
        members = sizes[axis]
        if dim is None:
            shape = (members,) + array.shape
        elif isinstance(dim, tuple):
            shape = (members, dim[2] + dim[1]) + array.shape[1:]
        else:
            shape = tuple(n * members if i == dim else n for i, n in enumerate(array.shape))
        shapes.append(jax.ShapeDtypeStruct(shape, array.dtype))
        whole = pltpu.VMEM(array.shape, array.dtype)
        if kind == "direct":
            scratch += [dma((members - 1,))] * 2 + [whole, dma((2,))]
        elif kind == "line":
            if isinstance(dim, tuple):
                whole = pltpu.VMEM(dim[1:2] + array.shape[1:], array.dtype)
            scratch += [dma((members // 2,))] * 5 + [whole, dma((2,))]
        else:
            scratch += [dma((members // 2,))] * 5 + [dma((members,))] * 5
            for _, length in cut(array.shape[0]):
                scratch += [pltpu.VMEM((length,) + array.shape[1:], array.dtype), dma((2,))]
    return pl.pallas_call(
        functools.partial(gather_kernel, plan, sizes),
        out_shape=tuple(shapes),
        in_specs=[pl.BlockSpec(memory_space=memory)] * len(arrays),
        out_specs=tuple([pl.BlockSpec(memory_space=memory)] * len(arrays)),
        scratch_shapes=scratch,
        compiler_params=pltpu.CompilerParams(collective_id=collective_id, has_side_effects=True),
    )(*arrays)


def local(
    sizes,
    tokens,
    row_lengths,
    attn_gain,
    query_weight,
    key_weight,
    value_matrix,
    output_weight,
    final_gain,
    value_head,
):
    width = tokens.shape[1] * sizes["tp"]
    rows_here = tokens.shape[0]
    head_cols = query_weight.shape[1]
    kv_cols = key_weight.shape[1]
    xfloat = tokens.astype(jnp.float32)
    squares_here = jnp.sum(xfloat * xfloat, axis=1)[None, :]
    gained = (xfloat * attn_gain).astype(jnp.bfloat16)
    packed = jnp.concatenate([query_weight, key_weight, value_matrix], axis=1)
    first = output_weight.shape[0] // 16
    early = output_weight.shape[0] // 4
    columns, weights, out_first, squares_all = gather(
        (
            ("split", "tp", 1),
            ("line", "rep", 0),
            ("line", "rep", (0, first, 0)),
            ("direct", "tp", None),
        ),
        sizes,
        (gained, packed, output_weight, squares_here),
        0,
    )
    first_scale = lax.rsqrt(jnp.sum(squares_all, axis=(0, 1)) / width + EPS)[:, None]
    projected = jnp.dot(columns, weights, preferred_element_type=jnp.float32)
    projected = (projected * first_scale).astype(jnp.bfloat16)
    query = projected[:, :head_cols]
    kv_all, out_early = gather(
        (("line", "tp", None), ("line", "rep", (first, early, 0))),
        sizes,
        (projected[:, head_cols:], output_weight),
        1,
    )
    sequence_rows = row_lengths.shape[0]
    length = rows_here // sequence_rows
    local_heads = head_cols // HEAD_SIZE
    key_full = kv_all[:, :, :kv_cols].transpose(1, 0, 2).reshape(rows_here, -1)
    value_full = kv_all[:, :, kv_cols:].transpose(1, 0, 2).reshape(rows_here, -1)
    first_head = lax.axis_index("tp") * local_heads
    key_value_index = (first_head + jnp.arange(local_heads, dtype=jnp.int32)) % KEY_VALUE_HEADS
    query4 = query.reshape(sequence_rows, length, local_heads, HEAD_SIZE)
    key4 = key_full.reshape(sequence_rows, length, KEY_VALUE_HEADS, HEAD_SIZE)
    value4 = value_full.reshape(sequence_rows, length, KEY_VALUE_HEADS, HEAD_SIZE)
    if local_heads % KEY_VALUE_HEADS or local_heads != KEY_VALUE_HEADS:
        key4 = jnp.take(key4, key_value_index, axis=2)
        value4 = jnp.take(value4, key_value_index, axis=2)
    scores = jnp.einsum(
        "rqhd,rkhd->rhqk", query4, key4, preferred_element_type=jnp.float32
    ) * (1.0 / HEAD_SIZE**0.5)
    position = jnp.arange(length, dtype=jnp.int32)
    causal = position[None, :] <= position[:, None]
    allowed = causal[None, None, :, :] & (
        position[None, None, None, :] < row_lengths[:, None, None, None]
    )
    scores = jnp.where(allowed, scores, jnp.float32(-1e30))
    scores = scores - jnp.max(scores, axis=3, keepdims=True)
    expo = jnp.exp(scores)
    probs = (expo / jnp.sum(expo, axis=3, keepdims=True)).astype(jnp.bfloat16)
    attended = jnp.einsum(
        "rhqk,rkhd->rqhd", probs, value4, preferred_element_type=jnp.float32
    )
    attended = attended.astype(jnp.bfloat16).reshape(rows_here, head_cols)
    before = first + early
    late = (before, output_weight.shape[0] - before, before)
    mixed, out_weights, _, _ = gather(
        (("split", "tp", 1), ("line", "rep", late), ("fill", 0, 1), ("fill", first, 1)),
        sizes,
        (attended, output_weight, out_first, out_early),
        2,
    )
    out_weights = out_weights.reshape(-1, tokens.shape[1])
    update = jnp.dot(mixed, out_weights, preferred_element_type=jnp.float32)
    resid_out = (xfloat + update).astype(jnp.bfloat16)
    rfloat = resid_out.astype(jnp.float32)
    squares = jnp.sum(rfloat * rfloat, axis=1)
    local_scores = jnp.dot(rfloat * final_gain, value_head, precision=lax.Precision.HIGHEST)
    stats = jnp.concatenate([local_scores.T, squares[None, :]], axis=0)
    (stats_all,) = gather((("direct", "tp", None),), sizes, (stats,), 3)
    stats = jnp.sum(stats_all, axis=0)
    logits = (stats[:-1] * lax.rsqrt(stats[-1:] / width + EPS)).T
    live = (position[None, :] < row_lengths[:, None]).reshape(rows_here, 1)
    objective_scores = jnp.where(live, logits, jnp.float32(0.0))
    return (resid_out, objective_scores)


UP, DOWN = True, False


class Pool:
    def __init__(self, ref):
        self.ref, self.used = ref, 0

    def take(self, number):
        base = self.used
        self.used += number
        return lambda index: self.ref.at[base + index]


class Route:
    def __init__(self, axis, size, span, pool):
        self.axis, self.span, self.size, self.count = axis, span, size, size // 2
        self.me = lax.axis_index(axis)
        self.place, self.side = self.me // 2, self.me % 2
        self.partner = self.me + 1 - 2 * self.side
        self.has_up = self.place < self.count - 1
        self.has_down = self.place > 0
        self.ready = False
        self.make(pool)

    def need(self):
        if not self.ready:
            self.ready = True
            self.gathered()

    def arrive(self):
        self.hop(1, UP)
        self.hop(1, DOWN)

    def copy(self, first, number, send, recv, target):
        return pltpu.make_async_remote_copy(
            src_ref=self.span(first, number),
            dst_ref=self.span(first, number),
            send_sem=send,
            recv_sem=recv,
            device_id={self.axis: target},
            device_id_type=MESH,
        )

    def sent(self, sem, number_at):
        numbers = [number_at(place) for place in range(self.count)]
        for number in sorted(set(numbers) - {0}):
            here = self.place < 0
            for place, other in enumerate(numbers):
                if other == number:
                    here = here | (self.place == place)
            pl.when(here)(lambda: self.copy(0, number, sem, sem, self.partner).wait_send())

    def ups(self, place):
        return place + 1 if place < self.count - 1 else 0

    def downs(self, place):
        return self.count - place if place > 0 else 0


class Row(Route):
    def make(self, pool):
        self.line_sem, self.pair_sem, self.pair_recv = pool.take(1)(0), pool.take(1)(0), pool.take(1)(0)
        self.line_recv = pool.take(self.count - 1)

    def up(self, origin):
        index = 2 * origin + self.side
        return self.copy(index, 1, self.line_sem, self.line_recv(origin), self.me + 2)

    def down(self, origin):
        index = 2 * origin + self.side
        return self.copy(index, 1, self.line_sem, self.line_recv(origin - 1), self.me - 2)

    def pair(self, origin):
        index = 2 * origin + self.side
        return self.copy(index, 1, self.pair_sem, self.pair_recv, self.partner)

    def begin(self):
        pl.when(self.has_up)(lambda: self.up(self.place).start())
        pl.when(self.has_down)(lambda: self.down(self.place).start())
        self.pair(self.place).start()

    def hop(self, step, upward):
        origin = self.place - step if upward else self.place + step

        @pl.when((origin >= 0) & (origin < self.count))
        def _():
            if upward:
                self.up(origin).wait_recv()
                pl.when(self.has_up)(lambda: self.up(origin).start())
            else:
                self.down(origin).wait_recv()
                pl.when(self.has_down)(lambda: self.down(origin).start())
            self.pair(origin).start()

    def gathered(self):
        self.copy(0, self.count, self.pair_sem, self.pair_recv, self.partner).wait_recv()

    def drain(self):
        self.copy(0, self.count, self.pair_sem, self.pair_recv, self.partner).wait_send()
        self.sent(self.line_sem, lambda place: self.ups(place) + self.downs(place))


class Crossed(Route):
    def make(self, pool):
        self.up_sem, self.down_sem = pool.take(1)(0), pool.take(1)(0)
        self.pair_sem, self.pair_recv = pool.take(1)(0), pool.take(1)(0)
        self.line_recv = pool.take(self.count - 1)

    def up(self, origin):
        return self.copy(2 * origin, 2, self.up_sem, self.line_recv(origin), self.me + 2)

    def down(self, origin):
        return self.copy(2 * origin, 2, self.down_sem, self.line_recv(origin - 1), self.me - 2)

    def across(self, index):
        return self.copy(index, 1, self.pair_sem, self.pair_recv, self.partner)

    def begin(self):
        self.across(self.me).start()

    def turn(self):
        self.across(self.partner).wait_recv()
        pl.when(self.has_up)(lambda: self.up(self.place).start())
        pl.when(self.has_down)(lambda: self.down(self.place).start())

    def hop(self, step, upward):
        origin = self.place - step if upward else self.place + step

        @pl.when((origin >= 0) & (origin < self.count))
        def _():
            if upward:
                self.up(origin).wait_recv()
                pl.when(self.has_up)(lambda: self.up(origin).start())
            else:
                self.down(origin).wait_recv()
                pl.when(self.has_down)(lambda: self.down(origin).start())

    def gathered(self):
        pass

    def drain(self):
        self.across(self.me).wait_send()
        self.sent(self.up_sem, lambda place: 2 * self.ups(place))
        self.sent(self.down_sem, lambda place: 2 * self.downs(place))


class Everyone:
    def __init__(self, axis, size, span, pool):
        self.axis, self.size, self.span = axis, size, span
        self.me = lax.axis_index(axis)
        self.send, self.recv = pool.take(1)(0), pool.take(1)(0)

    def copy(self, first, number, target):
        return pltpu.make_async_remote_copy(
            src_ref=self.span(first, number),
            dst_ref=self.span(first, number),
            send_sem=self.send,
            recv_sem=self.recv,
            device_id={self.axis: target},
            device_id_type=MESH,
        )

    def begin(self):
        for offset in range(1, self.size):
            self.copy(self.me, 1, lax.rem(self.me + offset, self.size)).start()

    def all(self):
        return self.copy(0, self.size - 1, lax.rem(self.me + 1, self.size))

    def gathered(self):
        self.all().wait_recv()

    def drain(self):
        self.all().wait_send()


NT = (((1,), (1,)), ((), ()))


def dot(a, b):
    return jnp.dot(a, b, preferred_element_type=jnp.float32)


def dot_nt(a, b):
    return lax.dot_general(a, b, NT, preferred_element_type=jnp.float32)


def exact_parts(values, number):
    parts = []
    for _ in range(number):
        part = values.astype(jnp.bfloat16)
        parts.append(part)
        values = values - part.astype(jnp.float32)
    return parts


def row_sums_of_squares(block):
    wide = block.astype(jnp.float32)
    ones = jnp.ones((16, block.shape[1]), jnp.bfloat16)
    high, low = exact_parts(wide * wide, 2)
    return (dot_nt(ones, high) + dot_nt(ones, low))[:8]


def layer_kernel(
    sizes,
    lengths_s,
    tokens_h,
    gain_h,
    query_h,
    key_h,
    value_h,
    output_h,
    final_h,
    head_h,
    resid_h,
    score_h,
    tok_all,
    wkv_all,
    wq_all,
    wo_all,
    kv_all,
    att_all,
    sq_all,
    stat_all,
    raw,
    gain,
    fgain,
    heads,
    judge,
    qbuf,
    resid,
    score,
    dma,
    local_dma,
):
    tp, rep = sizes["tp"], sizes["rep"]
    me_t, me_r = lax.axis_index("tp"), lax.axis_index("rep")
    pool, here = Pool(dma), Pool(local_dma)
    width = tp * tokens_h.shape[1]
    features = tokens_h.shape[1]
    sequences = lengths_s.shape[0]
    length = tokens_h.shape[0] // sequences
    kv_cols = key_h.shape[0]
    per_rep = tp // rep
    q_steps, q_cols = wq_all.shape[0], wq_all.shape[3]
    o_steps, o_cols = wo_all.shape[0], wo_all.shape[3]
    head_cols = q_steps * q_cols
    per_head = HEAD_SIZE // kv_cols
    crossing = length // (6 * 16) * 16

    def fetch(src, dst):
        made = pltpu.make_async_copy(src, dst, here.take(1)(0))
        made.start()
        return made

    def rows_of(s):
        return pl.ds(s * length, length)

    def gather_rows(buffer, s):
        start = s * length
        straight = pl.ds(start, length - crossing)
        rest = pl.ds(start + length - crossing, crossing)
        return [
            Crossed("tp", tp, lambda i, n: buffer(pl.ds(i, n), rest), pool),
            Row("tp", tp, lambda i, n: buffer(pl.ds(i, n), straight), pool),
        ]

    tok = [gather_rows(lambda i, r: tok_all.at[i, r], s) for s in range(sequences)]
    att = [
        [gather_rows(lambda i, r, j=j: att_all.at[j, i, r], s) for j in range(q_steps)]
        for s in range(sequences)
    ]
    kv = [Row("tp", tp, lambda i, n, s=s: kv_all.at[s, pl.ds(i, n)], pool) for s in range(sequences)]
    stat = Everyone("tp", tp, lambda i, n: stat_all.at[pl.ds(i, n)], pool)
    sq = Row("tp", tp, lambda i, n: sq_all.at[pl.ds(i, n)], pool)
    wkv = Row("rep", rep, lambda i, n: wkv_all.at[pl.ds(i, n)], pool)
    wq = [
        Row("rep", rep, lambda i, m, j=j: wq_all.at[j, pl.ds(i, m)], pool) for j in range(q_steps)
    ]
    wo = [
        Row("rep", rep, lambda i, m, n=n: wo_all.at[n, pl.ds(i, m)], pool) for n in range(o_steps)
    ]
    assert pool.used <= SEMAPHORES
    barrier = pltpu.get_barrier_semaphore()
    expected = 0
    for route in (sq, wkv):
        for there, target in (
            (route.has_up, route.me + 2),
            (route.has_down, route.me - 2),
            (route.place >= 0, route.partner),
        ):
            expected = expected + there.astype(jnp.int32)

            @pl.when(there)
            def _(axis=route.axis, target=target):
                pl.semaphore_signal(
                    barrier, inc=1, device_id={axis: target}, device_id_type=MESH
                )

    load_kv = [
        fetch(key_h, wkv_all.at[me_r, pl.ds(0, kv_cols)]),
        fetch(value_h, wkv_all.at[me_r, pl.ds(kv_cols, kv_cols)]),
    ]
    load_tokens = [fetch(gain_h, gain), fetch(tokens_h, raw)]
    load_q = [
        fetch(query_h.at[:, pl.ds(j * q_cols, q_cols)], wq_all.at[j, me_r]) for j in range(q_steps)
    ]
    load_o = [
        fetch(output_h.at[:, pl.ds(n * o_cols, o_cols)], wo_all.at[n, me_r]) for n in range(o_steps)
    ]
    load_final = [fetch(final_h, fgain), fetch(head_h, heads)]

    for copy in load_kv + load_tokens:
        copy.wait()
    for s in range(sequences):
        block = raw[rows_of(s), :].astype(jnp.float32) * gain[...]
        tok_all[me_t, rows_of(s), :] = block.astype(jnp.bfloat16)
    pl.semaphore_wait(barrier, expected)
    wkv.begin()
    for copy, job in zip(load_q, wq):
        copy.wait()
        job.begin()
    tok[0][0].begin()
    sq_all[me_t] = row_sums_of_squares(raw[...])
    sq.begin()
    tok[0][1].begin()
    for copy, job in zip(load_o, wo):
        copy.wait()
        job.begin()
    for copy in load_final:
        copy.wait()

    def row_scale(s):
        total = sq_all[0, :, rows_of(s)]
        for t in range(1, tp):
            total = total + sq_all[t, :, rows_of(s)]
        return lax.rsqrt(total / width + EPS)

    def project_kv(s):
        for job in tok[s] + [wkv, sq]:
            job.need()
        total = jnp.zeros((2 * kv_cols, length), jnp.float32)
        for t in range(tp):
            weight = wkv_all[t // per_rep, :, pl.ds(t % per_rep * features, features)]
            total = total + dot_nt(weight, tok_all[t, rows_of(s), :])
        kv_all[s, me_t] = (total * row_scale(s)[:1]).astype(jnp.bfloat16)
        kv[s].begin()

    def project_q(s, j):
        wq[j].need()
        total = jnp.zeros((length, q_cols), jnp.float32)
        for t in range(tp):
            weight = wq_all[j, t // per_rep, pl.ds(t % per_rep * features, features), :]
            total = total + dot(tok_all[t, rows_of(s), :], weight)
        column = row_scale(s).T[:, :1]
        qbuf[s, :, pl.ds(j * q_cols, q_cols)] = (total * column).astype(jnp.bfloat16)

    def attend(s, j):
        kv[s].need()
        here_length = lengths_s[s]
        query_at = lax.broadcasted_iota(jnp.int32, (length, length), 0)
        key_at = lax.broadcasted_iota(jnp.int32, (length, length), 1)
        allowed = (key_at <= query_at) & (key_at < here_length)
        for i in range(q_cols // HEAD_SIZE):
            h = j * (q_cols // HEAD_SIZE) + i
            first = h % KEY_VALUE_HEADS * per_head
            blocks = [kv_all[s, first + b] for b in range(per_head)]
            keys = jnp.concatenate([b[:kv_cols] for b in blocks], axis=0)
            values = jnp.concatenate([b[kv_cols:] for b in blocks], axis=0)
            query = qbuf[s, :, pl.ds(h * HEAD_SIZE, HEAD_SIZE)]
            scores = dot(query, keys) * (1.0 / HEAD_SIZE**0.5)
            scores = jnp.where(allowed, scores, jnp.float32(-1e30))
            expo = jnp.exp(scores - jnp.max(scores, axis=1, keepdims=True))
            probs = (expo / jnp.sum(expo, axis=1, keepdims=True)).astype(jnp.bfloat16)
            mixed = dot_nt(probs, values).astype(jnp.bfloat16)
            att_all[j, me_t, rows_of(s), pl.ds(i * HEAD_SIZE, HEAD_SIZE)] = mixed
        for job in att[s][j]:
            job.begin()

    def out_block(s, n):
        rows = pl.ds(pl.multiple_of(s * length, length), length)
        cols = pl.ds(pl.multiple_of(n * o_cols, o_cols), o_cols)
        update = jnp.zeros((length, o_cols), jnp.float32)
        for t in range(tp):
            for j in range(q_steps):
                weight = wo_all[n, t // per_rep, pl.ds(t % per_rep * head_cols + j * q_cols, q_cols), :]
                update = update + dot(att_all[j, t, rows, :], weight)
        block = (raw[rows, cols].astype(jnp.float32) + update).astype(jnp.bfloat16)
        resid[rows, cols] = block
        sums = dot_nt(judge[:, cols], block)
        sums = sums[0:8] + sums[8:16] + sums[16:24]
        line = lax.broadcasted_iota(jnp.int32, sums.shape, 0)
        sums = jnp.where(line == 7, row_sums_of_squares(block), sums)
        stat_all[me_t, s] += sums
        return 0

    def project_out(s):
        for job in sum(att[s], wo[:-1]):
            job.need()
        lax.fori_loop(0, o_steps - 1, lambda n, _: out_block(s, n), 0)

    def project_last():
        wo[-1].need()
        lax.fori_loop(0, sequences, lambda s, _: out_block(s, o_steps - 1), 0)

    def judges():
        weight = heads[...] * fgain[...]
        rest = jnp.zeros((8 - heads.shape[0], features), jnp.float32)
        weight = jnp.concatenate([weight, rest], axis=0)
        parts = [p.astype(jnp.float32) for p in exact_parts(weight, 3)]
        stat_all[me_t] = jnp.zeros(stat_all.shape[1:], jnp.float32)
        judge[...] = jnp.concatenate(parts + [jnp.zeros_like(weight)], axis=0).astype(jnp.bfloat16)

    def conclude(s):
        total = stat_all[0, s]
        for t in range(1, tp):
            total = total + stat_all[t, s]
        lane = lax.broadcasted_iota(jnp.int32, total.shape, 1)
        logits = total * lax.rsqrt(total[7:8] / width + EPS)
        return jnp.where(lane < lengths_s[s], logits, jnp.float32(0.0))

    tok[1][0].begin()
    sq.hop(1, DOWN)
    tok[1][1].begin()
    tok[0][1].hop(1, DOWN)
    tok[0][0].turn()
    tok[0][1].hop(1, UP)
    sq.hop(1, UP)
    sq.hop(2, DOWN)
    tok[0][1].hop(2, DOWN)
    tok[0][0].hop(1, UP)
    tok[0][1].hop(2, UP)
    tok[1][1].hop(1, UP)
    tok[0][1].hop(3, UP)
    judges()
    wkv.arrive()
    sq.hop(2, UP)
    tok[1][1].hop(1, DOWN)
    sq.hop(3, DOWN)
    tok[0][1].hop(3, DOWN)
    tok[0][0].hop(2, UP)
    sq.hop(3, UP)
    tok[0][0].hop(3, UP)
    tok[0][0].hop(1, DOWN)
    tok[0][0].hop(2, DOWN)
    wq[0].arrive()
    tok[1][1].hop(2, UP)
    tok[1][1].hop(2, DOWN)
    tok[1][0].turn()
    tok[0][0].hop(3, DOWN)
    project_kv(0)
    tok[1][1].hop(3, DOWN)
    tok[1][1].hop(3, UP)
    tok[1][0].hop(1, DOWN)
    kv[0].hop(1, UP)
    tok[1][0].hop(1, UP)
    kv[0].hop(1, DOWN)
    kv[0].hop(2, UP)
    wq[1].arrive()
    tok[1][0].hop(2, UP)
    kv[0].hop(2, DOWN)
    tok[1][0].hop(2, DOWN)
    kv[0].hop(3, UP)
    project_q(0, 1)
    project_q(0, 0)
    kv[0].hop(3, DOWN)
    tok[1][0].hop(3, UP)
    tok[1][0].hop(3, DOWN)
    project_kv(1)
    attend(0, 1)
    attend(0, 0)
    kv[1].hop(1, UP)
    project_q(1, 1)
    kv[1].hop(1, DOWN)
    att[0][1][1].hop(1, DOWN)
    kv[1].hop(2, DOWN)
    att[0][1][0].turn()
    kv[1].hop(3, DOWN)
    kv[1].hop(2, UP)
    att[0][0][1].hop(1, UP)
    att[0][0][1].hop(1, DOWN)
    project_q(1, 0)
    kv[1].hop(3, UP)
    att[0][1][1].hop(1, UP)
    wo[0].arrive()
    att[0][0][0].turn()
    att[0][0][1].hop(2, UP)
    att[0][1][1].hop(2, UP)
    att[0][1][1].hop(2, DOWN)
    att[0][1][0].hop(1, UP)
    attend(1, 0)
    attend(1, 1)
    att[0][1][0].hop(2, UP)
    att[0][1][1].hop(3, UP)
    att[0][0][1].hop(2, DOWN)
    wo[1].arrive()
    att[0][0][1].hop(3, UP)
    att[1][0][1].hop(1, DOWN)
    att[1][0][1].hop(1, UP)
    att[1][1][0].turn()
    att[0][0][0].hop(1, UP)
    att[0][1][0].hop(1, DOWN)
    att[1][1][1].hop(1, UP)
    att[1][0][1].hop(2, DOWN)
    att[1][1][1].hop(1, DOWN)
    att[1][0][1].hop(3, DOWN)
    att[1][1][0].hop(1, DOWN)
    att[1][1][1].hop(2, UP)
    att[0][0][1].hop(3, DOWN)
    att[0][0][0].hop(2, UP)
    att[0][1][1].hop(3, DOWN)
    att[0][1][0].hop(3, UP)
    att[0][0][0].hop(1, DOWN)
    att[1][0][0].turn()
    att[1][0][1].hop(2, UP)
    att[1][1][1].hop(2, DOWN)
    att[0][0][0].hop(2, DOWN)
    att[1][0][0].hop(1, UP)
    att[1][1][0].hop(1, UP)
    att[1][0][0].hop(1, DOWN)
    att[1][1][0].hop(2, DOWN)
    att[1][1][1].hop(3, UP)
    wo[2].arrive()
    att[0][0][0].hop(3, DOWN)
    att[1][1][1].hop(3, DOWN)
    att[1][0][1].hop(3, UP)
    att[0][1][0].hop(2, DOWN)
    att[0][0][0].hop(3, UP)
    att[1][0][0].hop(2, UP)
    att[1][1][0].hop(3, DOWN)
    att[1][1][0].hop(2, UP)
    att[0][1][0].hop(3, DOWN)
    project_out(0)
    att[1][0][0].hop(2, DOWN)
    att[1][0][0].hop(3, UP)
    wo[3].arrive()
    att[1][1][0].hop(3, UP)
    att[1][0][0].hop(3, DOWN)
    project_out(1)
    project_last()
    stat.begin()
    writes = [fetch(resid, resid_h)]
    for job in sum(tok + sum(att, []), []) + kv + [sq, wkv] + wq + wo:
        job.drain()
    stat.gathered()
    lines = [conclude(s) for s in range(sequences)]
    score[...] = jnp.concatenate(lines, axis=1)[: score.shape[0]]
    writes.append(fetch(score, score_h))
    stat.drain()
    for copy in writes:
        copy.wait()


def pass_on_kernel(pieces, resid_in, score_in, resid_out, score_out, resid, score, sems):
    rows = resid.shape[0] // pieces
    parts = [slice(i * rows, (i + 1) * rows) for i in range(pieces)]
    sources = [score_in] + [resid_in.at[p] for p in parts]
    places = [score] + [resid.at[p] for p in parts]
    targets = [score_out] + [resid_out.at[p] for p in parts]
    into = [
        pltpu.make_async_copy(a, b, sems.at[0, i]) for i, (a, b) in enumerate(zip(sources, places))
    ]
    out = [
        pltpu.make_async_copy(a, b, sems.at[1, i]) for i, (a, b) in enumerate(zip(places, targets))
    ]
    for copy in into:
        copy.start()
    for first, second in zip(into, out):
        first.wait()
        second.start()
    for copy in out:
        copy.wait()


def hand_over(resid, score):
    pieces = 4
    anywhere = pl.BlockSpec(memory_space=pl.ANY)
    return pl.pallas_call(
        functools.partial(pass_on_kernel, pieces),
        out_shape=tuple(jax.ShapeDtypeStruct(a.shape, a.dtype) for a in (resid, score)),
        in_specs=[anywhere] * 2,
        out_specs=(anywhere,) * 2,
        scratch_shapes=[
            pltpu.VMEM(resid.shape, resid.dtype),
            pltpu.VMEM(score.shape, score.dtype),
            pltpu.SemaphoreType.DMA((2, pieces + 1)),
        ],
    )(resid, score)


def whole_layer(
    sizes,
    tokens,
    row_lengths,
    attn_gain,
    query_weight,
    key_weight,
    value_matrix,
    output_weight,
    final_gain,
    value_head,
):
    tp, rep = sizes["tp"], sizes["rep"]
    rows, features = tokens.shape
    sequences = row_lengths.shape[0]
    length = rows // sequences
    depth, head_cols = query_weight.shape
    kv_cols = key_weight.shape[1]
    mixed = output_weight.shape[0]
    vmem, dma = pltpu.VMEM, pltpu.SemaphoreType.DMA
    half, single = jnp.bfloat16, jnp.float32
    q_steps, o_steps = head_cols // STEP, features // STEP
    anywhere = pl.BlockSpec(memory_space=pl.ANY)
    resid, score = pl.pallas_call(
        functools.partial(layer_kernel, sizes),
        out_shape=(
            jax.ShapeDtypeStruct((rows, features), half),
            jax.ShapeDtypeStruct((value_head.shape[1], rows), single),
        ),
        in_specs=[pl.BlockSpec(memory_space=pltpu.SMEM)] + [pl.BlockSpec(memory_space=pltpu.HBM)] * 8,
        out_specs=(anywhere, anywhere),
        scratch_shapes=[
            vmem((tp, rows, features), half),
            vmem((rep, 2 * kv_cols, depth), half),
            vmem((q_steps, rep, depth, STEP), half),
            vmem((o_steps, rep, mixed, STEP), half),
            vmem((sequences, tp, 2 * kv_cols, length), half),
            vmem((q_steps, tp, rows, STEP), half),
            vmem((tp, 8, rows), single),
            vmem((tp, sequences, 8, length), single),
            vmem((rows, features), half),
            vmem((1, features), single),
            vmem((1, features), single),
            vmem((value_head.shape[1], features), single),
            vmem((32, features), half),
            vmem((sequences, length, head_cols), half),
            vmem((rows, features), half),
            vmem((value_head.shape[1], rows), single),
            dma((SEMAPHORES,)),
            dma((16,)),
        ],
        compiler_params=pltpu.CompilerParams(
            collective_id=4, has_side_effects=True, vmem_limit_bytes=64 * 1024 * 1024 - 128 * 1024
        ),
    )(
        row_lengths,
        tokens,
        attn_gain[None, :],
        query_weight,
        key_weight.T,
        value_matrix.T,
        output_weight,
        final_gain[None, :],
        value_head.T,
    )
    resid, score = hand_over(resid, score)
    return resid, score.T


def fits(sizes, tokens, row_lengths, query_weight, key_weight):
    heads = query_weight.shape[1] // HEAD_SIZE
    return (
        row_lengths.shape[0] == 2
        and sizes["rep"] == 4
        and sizes["tp"] % sizes["rep"] == 0
        and sizes["tp"] == 8
        and heads > 0
        and heads % KEY_VALUE_HEADS == 0
        and query_weight.shape[1] == 2 * STEP
        and tokens.shape[1] == 4 * STEP
        and HEAD_SIZE % key_weight.shape[1] == 0
    )


def layer(sizes, tokens, row_lengths, attn_gain, query_weight, key_weight, *rest):
    chosen = whole_layer if fits(sizes, tokens, row_lengths, query_weight, key_weight) else local
    return chosen(sizes, tokens, row_lengths, attn_gain, query_weight, key_weight, *rest)


def solution(mesh):
    in_specs = (
        P("rep", "tp"),
        P("rep"),
        P("tp"),
        P("rep", "tp"),
        P("rep", "tp"),
        P("rep", "tp"),
        P("rep", "tp"),
        P("tp"),
        P("tp", None),
    )
    out_specs = (P("rep", "tp"), P("rep", None))
    body = functools.partial(layer, dict(mesh.shape))
    return jax.shard_map(body, mesh=mesh, in_specs=in_specs, out_specs=out_specs, check_vma=False)
```

```python
import functools
import jax
import jax.numpy as jnp
from jax import lax
from jax.experimental import pallas as pl
from jax.experimental.pallas import tpu as pltpu
from jax.sharding import PartitionSpec as P

KEY_VALUE_HEADS = 4
HEAD_SIZE = 128
EPS = 1e-05
MESH = pl.DeviceIdType.MESH
STEP = 256
SEMAPHORES = 126


class Stage:
    def __init__(self, src, dst, buffer, sems):
        self.into = pltpu.make_async_copy(src, buffer, sems.at[0])
        self.out = pltpu.make_async_copy(buffer, dst, sems.at[1])


def slot(ref, dim, size, index, rows=None):
    if rows is not None:
        return ref.at[pl.ds(*rows), pl.ds(pl.multiple_of(index * size, size), size)]
    if dim is None:
        return ref.at[index]
    if isinstance(dim, tuple):
        return ref.at[index, pl.ds(dim[2], dim[1])]
    start = pl.multiple_of(index * size, size)
    return ref.at[pl.ds(start, size)] if dim == 0 else ref.at[:, pl.ds(start, size)]


class Line:
    def __init__(self, axis, count, dim, src, dst, sems, rows=None):
        self.axis, self.dim, self.dst = axis, dim, dst
        self.windowed = isinstance(dim, tuple)
        rows = dim[:2] if self.windowed else rows
        self.src = src if rows is None else src.at[pl.ds(*rows)]
        self.rows = None if self.windowed else rows
        self.count = count
        self.up_sem, self.down_sem, self.pair_sem, self.line_recv, self.pair_recv = sems
        me = lax.axis_index(axis)
        self.me, self.place, self.side = me, me // 2, me % 2
        self.partner = me + 1 - 2 * self.side
        self.size = None if dim is None or self.windowed else src.shape[dim]

    def at(self, index):
        return slot(self.dst, self.dim, self.size, index, self.rows)

    def copy(self, source, index, send, recv, target):
        return pltpu.make_async_remote_copy(
            src_ref=source,
            dst_ref=self.at(index),
            send_sem=send,
            recv_sem=recv,
            device_id={self.axis: target},
            device_id_type=MESH,
        )

    def up(self, source, origin):
        return self.copy(
            source, 2 * origin + self.side, self.up_sem.at[origin], self.line_recv.at[origin], self.me + 2
        )

    def down(self, source, origin):
        return self.copy(
            source, 2 * origin + self.side, self.down_sem.at[origin], self.line_recv.at[origin], self.me - 2
        )

    def pair(self, source, origin):
        return self.copy(
            source,
            2 * origin + self.side,
            self.pair_sem.at[origin],
            self.pair_recv.at[origin],
            self.partner,
        )

    def own_block(self):
        return self.at(self.me)

    def has_up(self):
        return self.place < self.count - 1

    def has_down(self):
        return self.place > 0

    def begin(self):
        @pl.when(self.has_up())
        def _():
            self.up(self.src, self.place).start()

        @pl.when(self.has_down())
        def _():
            self.down(self.src, self.place).start()

        self.pair(self.src, self.place).start()

    def hop(self, step):
        below, above = self.place - step, self.place + step

        @pl.when(below >= 0)
        def _():
            block = self.at(2 * below + self.side)
            self.up(block, below).wait_recv()

            @pl.when(self.has_up())
            def _():
                self.up(block, below).start()

            self.pair(block, below).start()

        @pl.when(above < self.count)
        def _():
            block = self.at(2 * above + self.side)
            self.down(block, above).wait_recv()

            @pl.when(self.has_down())
            def _():
                self.down(block, above).start()

            self.pair(block, above).start()

    def finish(self):
        for origin in range(self.count):
            here = self.at(2 * origin + self.side)
            self.pair(here, origin).wait_send()
            pltpu.make_async_remote_copy(
                src_ref=here,
                dst_ref=self.at(2 * origin + 1 - self.side),
                send_sem=self.pair_sem.at[origin],
                recv_sem=self.pair_recv.at[origin],
                device_id={self.axis: self.partner},
                device_id_type=MESH,
            ).wait_recv()

            @pl.when((origin <= self.place) & self.has_up())
            def _():
                self.up(here, origin).wait_send()

            @pl.when((origin >= self.place) & self.has_down())
            def _():
                self.down(here, origin).wait_send()

    def neighbours(self):
        return ((self.has_up(), self.me + 2), (self.has_down(), self.me - 2), (None, self.partner))


class Cross(Line):
    def __init__(self, axis, count, dim, src, dst, sems, rows):
        super().__init__(axis, count, dim, src, dst, sems, rows)
        self.other = 1 - self.side

    def along(self, source, origin, side, which, step):
        sem = self.up_sem if step > 0 else self.down_sem
        return self.copy(
            source,
            2 * origin + side,
            sem.at[which * self.count + origin],
            self.line_recv.at[which * self.count + origin],
            self.me + step,
        )

    def spread(self, source, origin, which):
        side = self.side if which == 0 else self.other

        @pl.when(self.has_up() & (origin <= self.place))
        def _():
            self.along(source, origin, side, which, 2).start()

        @pl.when(self.has_down() & (origin >= self.place))
        def _():
            self.along(source, origin, side, which, -2).start()

    def across(self, index, source):
        return self.copy(source, index, self.pair_sem.at[0], self.pair_recv.at[0], self.partner)

    def begin(self):
        self.across(self.me, self.src).start()
        self.spread(self.src, self.place, 0)

    def turn(self):
        theirs = self.at(self.partner)
        self.across(self.partner, theirs).wait_recv()
        self.spread(theirs, self.place, 1)

    def hop(self, step):
        for which in range(2):
            side = self.side if which == 0 else self.other
            for origin in (self.place - step, self.place + step):

                @pl.when((origin >= 0) & (origin < self.count))
                def _(origin=origin, side=side, which=which):
                    block = self.at(2 * origin + side)
                    self.along(block, origin, side, which, 2).wait_recv()
                    self.spread(block, origin, which)

    def finish(self):
        self.across(self.me, self.src).wait_send()
        for which in range(2):
            side = self.side if which == 0 else self.other
            for origin in range(self.count):
                block = self.at(2 * origin + side)

                @pl.when((origin <= self.place) & self.has_up())
                def _(origin=origin, side=side, which=which, block=block):
                    self.along(block, origin, side, which, 2).wait_send()

                @pl.when((origin >= self.place) & self.has_down())
                def _(origin=origin, side=side, which=which, block=block):
                    self.along(block, origin, side, which, -2).wait_send()


class Direct:
    def __init__(self, axis, members, src, dst, sems):
        self.axis, self.members, self.src, self.dst = axis, members, src, dst
        self.send, self.recv = sems
        self.me = lax.axis_index(axis)

    def to(self, offset):
        return pltpu.make_async_remote_copy(
            src_ref=self.src,
            dst_ref=self.dst.at[self.me],
            send_sem=self.send.at[offset - 1],
            recv_sem=self.recv.at[offset - 1],
            device_id={self.axis: lax.rem(self.me + offset, self.members)},
            device_id_type=MESH,
        )

    def come(self, offset):
        return pltpu.make_async_remote_copy(
            src_ref=self.src,
            dst_ref=self.dst.at[lax.rem(self.me - offset + self.members, self.members)],
            send_sem=self.send.at[offset - 1],
            recv_sem=self.recv.at[offset - 1],
            device_id={self.axis: lax.rem(self.me + offset, self.members)},
            device_id_type=MESH,
        )

    def own_block(self):
        return self.dst.at[self.me]

    def begin(self):
        for offset in range(1, self.members):
            self.to(offset).start()

    def finish(self):
        for offset in range(1, self.members):
            self.to(offset).wait_send()
            self.come(offset).wait_recv()


def gather_kernel(plan, sizes, *refs):
    count = len(plan)
    sources, targets = refs[:count], refs[count : 2 * count]
    rest = list(refs[2 * count :])

    def take(number):
        taken = rest[:number]
        del rest[:number]
        return taken

    jobs, stages = [], []
    for (kind, axis, dim), src, dst in zip(plan, sources, targets):
        if kind == "fill":
            dst = targets[dim]
            buffer, sems = take(2)
            stages.append(Stage(src, dst.at[:, pl.ds(axis, src.shape[1])], buffer, sems))
            continue
        if kind == "direct":
            made = [Direct(axis, sizes[axis], src, dst, take(2))]
        elif kind == "line":
            made = [Line(axis, sizes[axis] // 2, dim, src, dst, take(5))]
        else:
            first, second = cut(src.shape[0])
            made = [
                Line(axis, sizes[axis] // 2, dim, src, dst, take(5), first),
                Cross(axis, sizes[axis] // 2, dim, src, dst, take(5), second),
            ]
        for job in made:
            buffer, sems = take(2)
            stages.append(Stage(job.src, job.own_block(), buffer, sems))
        jobs += made
    barrier = pltpu.get_barrier_semaphore()
    direct_axes = {job.axis for job in jobs if isinstance(job, Direct)}
    greeted, peers = set(), 0
    for job in jobs:
        if job.axis in greeted:
            continue
        greeted.add(job.axis)
        if job.axis in direct_axes:
            members = sizes[job.axis]
            peers = peers + members - 1
            for offset in range(1, members):
                pl.semaphore_signal(
                    barrier,
                    inc=1,
                    device_id={job.axis: lax.rem(job.me + offset, members)},
                    device_id_type=MESH,
                )
        else:
            for there, target in job.neighbours():
                def signal(target=target, job=job):
                    pl.semaphore_signal(
                        barrier, inc=1, device_id={job.axis: target}, device_id_type=MESH
                    )

                if there is None:
                    peers = peers + 1
                    signal()
                else:
                    peers = peers + there.astype(jnp.int32)
                    pl.when(there)(signal)
    pl.semaphore_wait(barrier, peers)
    for job in jobs:
        job.begin()
    for stage in stages:
        stage.into.start()
    for stage in stages:
        stage.into.wait()
        stage.out.start()
    for job in jobs:
        if isinstance(job, Cross):
            job.turn()
    for axis in ("tp", "rep"):
        lines = [job for job in jobs if isinstance(job, Line) and job.axis == axis]
        for step in range(1, max([job.count for job in lines], default=1)):
            for job in lines:
                job.hop(step)
    for job in jobs:
        job.finish()
    for stage in stages:
        stage.out.wait()


def cut(total):
    cross = total // (6 * 16) * 16
    return (0, total - cross), (total - cross, cross)


def gather(plan, sizes, arrays, collective_id, memory=pl.ANY):
    shapes, scratch = [], []
    dma = pltpu.SemaphoreType.DMA
    for (kind, axis, dim), array in zip(plan, arrays):
        if kind == "fill":
            shapes.append(jax.ShapeDtypeStruct((8, 128), array.dtype))
            scratch += [pltpu.VMEM(array.shape, array.dtype), dma((2,))]
            continue
        members = sizes[axis]
        if dim is None:
            shape = (members,) + array.shape
        elif isinstance(dim, tuple):
            shape = (members, dim[2] + dim[1]) + array.shape[1:]
        else:
            shape = tuple(n * members if i == dim else n for i, n in enumerate(array.shape))
        shapes.append(jax.ShapeDtypeStruct(shape, array.dtype))
        whole = pltpu.VMEM(array.shape, array.dtype)
        if kind == "direct":
            scratch += [dma((members - 1,))] * 2 + [whole, dma((2,))]
        elif kind == "line":
            if isinstance(dim, tuple):
                whole = pltpu.VMEM(dim[1:2] + array.shape[1:], array.dtype)
            scratch += [dma((members // 2,))] * 5 + [whole, dma((2,))]
        else:
            scratch += [dma((members // 2,))] * 5 + [dma((members,))] * 5
            for _, length in cut(array.shape[0]):
                scratch += [pltpu.VMEM((length,) + array.shape[1:], array.dtype), dma((2,))]
    return pl.pallas_call(
        functools.partial(gather_kernel, plan, sizes),
        out_shape=tuple(shapes),
        in_specs=[pl.BlockSpec(memory_space=memory)] * len(arrays),
        out_specs=tuple([pl.BlockSpec(memory_space=memory)] * len(arrays)),
        scratch_shapes=scratch,
        compiler_params=pltpu.CompilerParams(collective_id=collective_id, has_side_effects=True),
    )(*arrays)


def local(
    sizes,
    tokens,
    row_lengths,
    attn_gain,
    query_weight,
    key_weight,
    value_matrix,
    output_weight,
    final_gain,
    value_head,
):
    width = tokens.shape[1] * sizes["tp"]
    rows_here = tokens.shape[0]
    head_cols = query_weight.shape[1]
    kv_cols = key_weight.shape[1]
    xfloat = tokens.astype(jnp.float32)
    squares_here = jnp.sum(xfloat * xfloat, axis=1)[None, :]
    gained = (xfloat * attn_gain).astype(jnp.bfloat16)
    packed = jnp.concatenate([query_weight, key_weight, value_matrix], axis=1)
    first = output_weight.shape[0] // 16
    early = output_weight.shape[0] // 4
    columns, weights, out_first, squares_all = gather(
        (
            ("split", "tp", 1),
            ("line", "rep", 0),
            ("line", "rep", (0, first, 0)),
            ("direct", "tp", None),
        ),
        sizes,
        (gained, packed, output_weight, squares_here),
        0,
    )
    first_scale = lax.rsqrt(jnp.sum(squares_all, axis=(0, 1)) / width + EPS)[:, None]
    projected = jnp.dot(columns, weights, preferred_element_type=jnp.float32)
    projected = (projected * first_scale).astype(jnp.bfloat16)
    query = projected[:, :head_cols]
    kv_all, out_early = gather(
        (("line", "tp", None), ("line", "rep", (first, early, 0))),
        sizes,
        (projected[:, head_cols:], output_weight),
        1,
    )
    sequence_rows = row_lengths.shape[0]
    length = rows_here // sequence_rows
    local_heads = head_cols // HEAD_SIZE
    key_full = kv_all[:, :, :kv_cols].transpose(1, 0, 2).reshape(rows_here, -1)
    value_full = kv_all[:, :, kv_cols:].transpose(1, 0, 2).reshape(rows_here, -1)
    first_head = lax.axis_index("tp") * local_heads
    key_value_index = (first_head + jnp.arange(local_heads, dtype=jnp.int32)) % KEY_VALUE_HEADS
    query4 = query.reshape(sequence_rows, length, local_heads, HEAD_SIZE)
    key4 = key_full.reshape(sequence_rows, length, KEY_VALUE_HEADS, HEAD_SIZE)
    value4 = value_full.reshape(sequence_rows, length, KEY_VALUE_HEADS, HEAD_SIZE)
    if local_heads % KEY_VALUE_HEADS or local_heads != KEY_VALUE_HEADS:
        key4 = jnp.take(key4, key_value_index, axis=2)
        value4 = jnp.take(value4, key_value_index, axis=2)
    scores = jnp.einsum(
        "rqhd,rkhd->rhqk", query4, key4, preferred_element_type=jnp.float32
    ) * (1.0 / HEAD_SIZE**0.5)
    position = jnp.arange(length, dtype=jnp.int32)
    causal = position[None, :] <= position[:, None]
    allowed = causal[None, None, :, :] & (
        position[None, None, None, :] < row_lengths[:, None, None, None]
    )
    scores = jnp.where(allowed, scores, jnp.float32(-1e30))
    scores = scores - jnp.max(scores, axis=3, keepdims=True)
    expo = jnp.exp(scores)
    probs = (expo / jnp.sum(expo, axis=3, keepdims=True)).astype(jnp.bfloat16)
    attended = jnp.einsum(
        "rhqk,rkhd->rqhd", probs, value4, preferred_element_type=jnp.float32
    )
    attended = attended.astype(jnp.bfloat16).reshape(rows_here, head_cols)
    before = first + early
    late = (before, output_weight.shape[0] - before, before)
    mixed, out_weights, _, _ = gather(
        (("split", "tp", 1), ("line", "rep", late), ("fill", 0, 1), ("fill", first, 1)),
        sizes,
        (attended, output_weight, out_first, out_early),
        2,
    )
    out_weights = out_weights.reshape(-1, tokens.shape[1])
    update = jnp.dot(mixed, out_weights, preferred_element_type=jnp.float32)
    resid_out = (xfloat + update).astype(jnp.bfloat16)
    rfloat = resid_out.astype(jnp.float32)
    squares = jnp.sum(rfloat * rfloat, axis=1)
    local_scores = jnp.dot(rfloat * final_gain, value_head, precision=lax.Precision.HIGHEST)
    stats = jnp.concatenate([local_scores.T, squares[None, :]], axis=0)
    (stats_all,) = gather((("direct", "tp", None),), sizes, (stats,), 3)
    stats = jnp.sum(stats_all, axis=0)
    logits = (stats[:-1] * lax.rsqrt(stats[-1:] / width + EPS)).T
    live = (position[None, :] < row_lengths[:, None]).reshape(rows_here, 1)
    objective_scores = jnp.where(live, logits, jnp.float32(0.0))
    return (resid_out, objective_scores)


UP, DOWN = True, False


class Pool:
    def __init__(self, ref):
        self.ref, self.used = ref, 0

    def take(self, number):
        base = self.used
        self.used += number
        return lambda index: self.ref.at[base + index]


class Route:
    def __init__(self, axis, size, span, pool):
        self.axis, self.span, self.size, self.count = axis, span, size, size // 2
        self.me = lax.axis_index(axis)
        self.place, self.side = self.me // 2, self.me % 2
        self.partner = self.me + 1 - 2 * self.side
        self.has_up = self.place < self.count - 1
        self.has_down = self.place > 0
        self.ready = False
        self.make(pool)

    def need(self):
        if not self.ready:
            self.ready = True
            self.gathered()

    def arrive(self):
        self.hop(1, UP)
        self.hop(1, DOWN)

    def copy(self, first, number, send, recv, target):
        return pltpu.make_async_remote_copy(
            src_ref=self.span(first, number),
            dst_ref=self.span(first, number),
            send_sem=send,
            recv_sem=recv,
            device_id={self.axis: target},
            device_id_type=MESH,
        )

    def sent(self, sem, number_at):
        numbers = [number_at(place) for place in range(self.count)]
        for number in sorted(set(numbers) - {0}):
            here = self.place < 0
            for place, other in enumerate(numbers):
                if other == number:
                    here = here | (self.place == place)
            pl.when(here)(lambda: self.copy(0, number, sem, sem, self.partner).wait_send())

    def ups(self, place):
        return place + 1 if place < self.count - 1 else 0

    def downs(self, place):
        return self.count - place if place > 0 else 0


class Row(Route):
    def make(self, pool):
        self.line_sem, self.pair_sem, self.pair_recv = pool.take(1)(0), pool.take(1)(0), pool.take(1)(0)
        self.line_recv = pool.take(self.count - 1)

    def up(self, origin):
        index = 2 * origin + self.side
        return self.copy(index, 1, self.line_sem, self.line_recv(origin), self.me + 2)

    def down(self, origin):
        index = 2 * origin + self.side
        return self.copy(index, 1, self.line_sem, self.line_recv(origin - 1), self.me - 2)

    def pair(self, origin):
        index = 2 * origin + self.side
        return self.copy(index, 1, self.pair_sem, self.pair_recv, self.partner)

    def begin(self):
        pl.when(self.has_up)(lambda: self.up(self.place).start())
        pl.when(self.has_down)(lambda: self.down(self.place).start())
        self.pair(self.place).start()

    def hop(self, step, upward):
        origin = self.place - step if upward else self.place + step

        @pl.when((origin >= 0) & (origin < self.count))
        def _():
            if upward:
                self.up(origin).wait_recv()
                pl.when(self.has_up)(lambda: self.up(origin).start())
            else:
                self.down(origin).wait_recv()
                pl.when(self.has_down)(lambda: self.down(origin).start())
            self.pair(origin).start()

    def gathered(self):
        self.copy(0, self.count, self.pair_sem, self.pair_recv, self.partner).wait_recv()

    def drain(self):
        self.copy(0, self.count, self.pair_sem, self.pair_recv, self.partner).wait_send()
        self.sent(self.line_sem, lambda place: self.ups(place) + self.downs(place))


class Crossed(Route):
    def make(self, pool):
        self.up_sem, self.down_sem = pool.take(1)(0), pool.take(1)(0)
        self.pair_sem, self.pair_recv = pool.take(1)(0), pool.take(1)(0)
        self.line_recv = pool.take(self.count - 1)

    def up(self, origin):
        return self.copy(2 * origin, 2, self.up_sem, self.line_recv(origin), self.me + 2)

    def down(self, origin):
        return self.copy(2 * origin, 2, self.down_sem, self.line_recv(origin - 1), self.me - 2)

    def across(self, index):
        return self.copy(index, 1, self.pair_sem, self.pair_recv, self.partner)

    def begin(self):
        self.across(self.me).start()

    def turn(self):
        self.across(self.partner).wait_recv()
        pl.when(self.has_up)(lambda: self.up(self.place).start())
        pl.when(self.has_down)(lambda: self.down(self.place).start())

    def hop(self, step, upward):
        origin = self.place - step if upward else self.place + step

        @pl.when((origin >= 0) & (origin < self.count))
        def _():
            if upward:
                self.up(origin).wait_recv()
                pl.when(self.has_up)(lambda: self.up(origin).start())
            else:
                self.down(origin).wait_recv()
                pl.when(self.has_down)(lambda: self.down(origin).start())

    def gathered(self):
        pass

    def drain(self):
        self.across(self.me).wait_send()
        self.sent(self.up_sem, lambda place: 2 * self.ups(place))
        self.sent(self.down_sem, lambda place: 2 * self.downs(place))


class Everyone:
    def __init__(self, axis, size, span, pool):
        self.axis, self.size, self.span = axis, size, span
        self.me = lax.axis_index(axis)
        self.send, self.recv = pool.take(1)(0), pool.take(1)(0)

    def copy(self, first, number, target):
        return pltpu.make_async_remote_copy(
            src_ref=self.span(first, number),
            dst_ref=self.span(first, number),
            send_sem=self.send,
            recv_sem=self.recv,
            device_id={self.axis: target},
            device_id_type=MESH,
        )

    def begin(self):
        for offset in range(1, self.size):
            self.copy(self.me, 1, lax.rem(self.me + offset, self.size)).start()

    def all(self):
        return self.copy(0, self.size - 1, lax.rem(self.me + 1, self.size))

    def gathered(self):
        self.all().wait_recv()

    def drain(self):
        self.all().wait_send()


NT = (((1,), (1,)), ((), ()))


def dot(a, b):
    return jnp.dot(a, b, preferred_element_type=jnp.float32)


def dot_nt(a, b):
    return lax.dot_general(a, b, NT, preferred_element_type=jnp.float32)


def exact_parts(values, number):
    parts = []
    for _ in range(number):
        part = values.astype(jnp.bfloat16)
        parts.append(part)
        values = values - part.astype(jnp.float32)
    return parts


def row_sums_of_squares(block):
    wide = block.astype(jnp.float32)
    ones = jnp.ones((16, block.shape[1]), jnp.bfloat16)
    high, low = exact_parts(wide * wide, 2)
    return (dot_nt(ones, high) + dot_nt(ones, low))[:8]


def layer_kernel(
    sizes,
    lengths_s,
    tokens_h,
    gain_h,
    query_h,
    key_h,
    value_h,
    output_h,
    final_h,
    head_h,
    resid_h,
    score_h,
    tok_all,
    wkv_all,
    wq_all,
    wo_all,
    kv_all,
    att_all,
    sq_all,
    stat_all,
    stat_here,
    raw,
    gain,
    fgain,
    heads,
    judge,
    qbuf,
    resid,
    score,
    dma,
    local_dma,
):
    tp, rep = sizes["tp"], sizes["rep"]
    me_t, me_r = lax.axis_index("tp"), lax.axis_index("rep")
    pool, here = Pool(dma), Pool(local_dma)
    width = tp * tokens_h.shape[1]
    features = tokens_h.shape[1]
    sequences = lengths_s.shape[0]
    length = tokens_h.shape[0] // sequences
    kv_cols = key_h.shape[0]
    per_rep = tp // rep
    q_steps, q_cols = wq_all.shape[0], wq_all.shape[3]
    o_steps, o_cols = wo_all.shape[0], wo_all.shape[3]
    head_cols = q_steps * q_cols
    per_head = HEAD_SIZE // kv_cols
    crossing = length // (6 * 16) * 16

    def fetch(src, dst):
        made = pltpu.make_async_copy(src, dst, here.take(1)(0))
        made.start()
        return made

    def rows_of(s):
        return pl.ds(s * length, length)

    def gather_rows(buffer, s):
        start = s * length
        straight = pl.ds(start, length - crossing)
        rest = pl.ds(start + length - crossing, crossing)
        return [
            Crossed("tp", tp, lambda i, n: buffer(pl.ds(i, n), rest), pool),
            Row("tp", tp, lambda i, n: buffer(pl.ds(i, n), straight), pool),
        ]

    tok = [gather_rows(lambda i, r: tok_all.at[i, r], s) for s in range(sequences)]
    att = [
        [gather_rows(lambda i, r, j=j: att_all.at[j, i, r], s) for j in range(q_steps)]
        for s in range(sequences)
    ]
    kv = [Row("tp", tp, lambda i, n, s=s: kv_all.at[s, pl.ds(i, n)], pool) for s in range(sequences)]
    stat = Everyone("tp", tp, lambda i, n: stat_all.at[pl.ds(i, n)], pool)
    sq = Row("tp", tp, lambda i, n: sq_all.at[pl.ds(i, n)], pool)
    wkv = Row("rep", rep, lambda i, n: wkv_all.at[pl.ds(i, n)], pool)
    wq = [
        Row("rep", rep, lambda i, m, j=j: wq_all.at[j, pl.ds(i, m)], pool) for j in range(q_steps)
    ]
    wo = [
        Row("rep", rep, lambda i, m, n=n: wo_all.at[n, pl.ds(i, m)], pool) for n in range(o_steps)
    ]
    assert pool.used <= SEMAPHORES
    barrier = pltpu.get_barrier_semaphore()
    expected = 0
    for route in (sq, wkv):
        for there, target in (
            (route.has_up, route.me + 2),
            (route.has_down, route.me - 2),
            (route.place >= 0, route.partner),
        ):
            expected = expected + there.astype(jnp.int32)

            @pl.when(there)
            def _(axis=route.axis, target=target):
                pl.semaphore_signal(
                    barrier, inc=1, device_id={axis: target}, device_id_type=MESH
                )

    load_kv = [
        fetch(key_h, wkv_all.at[me_r, pl.ds(0, kv_cols)]),
        fetch(value_h, wkv_all.at[me_r, pl.ds(kv_cols, kv_cols)]),
    ]
    load_tokens = [fetch(gain_h, gain), fetch(tokens_h, raw)]
    load_q = [
        fetch(query_h.at[:, pl.ds(j * q_cols, q_cols)], wq_all.at[j, me_r]) for j in range(q_steps)
    ]
    load_o = [
        fetch(output_h.at[:, pl.ds(n * o_cols, o_cols)], wo_all.at[n, me_r]) for n in range(o_steps)
    ]
    load_final = [fetch(final_h, fgain), fetch(head_h, heads)]

    for copy in load_kv + load_tokens:
        copy.wait()
    for s in range(sequences):
        block = raw[rows_of(s), :].astype(jnp.float32) * gain[...]
        tok_all[me_t, rows_of(s), :] = block.astype(jnp.bfloat16)
    pl.semaphore_wait(barrier, expected)
    wkv.begin()
    for copy, job in zip(load_q, wq):
        copy.wait()
        job.begin()
    tok[0][0].begin()
    sq_all[me_t] = row_sums_of_squares(raw[...])
    sq.begin()
    tok[0][1].begin()
    for copy, job in zip(load_o, wo):
        copy.wait()
        job.begin()
    for copy in load_final:
        copy.wait()

    def row_scale(s):
        total = sq_all[0, :, rows_of(s)]
        for t in range(1, tp):
            total = total + sq_all[t, :, rows_of(s)]
        return lax.rsqrt(total / width + EPS)

    def project_kv(s):
        for job in tok[s] + [wkv, sq]:
            job.need()
        total = jnp.zeros((2 * kv_cols, length), jnp.float32)
        for t in range(tp):
            weight = wkv_all[t // per_rep, :, pl.ds(t % per_rep * features, features)]
            total = total + dot_nt(weight, tok_all[t, rows_of(s), :])
        kv_all[s, me_t] = (total * row_scale(s)[:1]).astype(jnp.bfloat16)
        kv[s].begin()

    def project_q(s, j):
        wq[j].need()
        total = jnp.zeros((length, q_cols), jnp.float32)
        for t in range(tp):
            weight = wq_all[j, t // per_rep, pl.ds(t % per_rep * features, features), :]
            total = total + dot(tok_all[t, rows_of(s), :], weight)
        column = row_scale(s).T[:, :1]
        qbuf[s, :, pl.ds(j * q_cols, q_cols)] = (total * column).astype(jnp.bfloat16)

    def attend(s, j):
        kv[s].need()
        here_length = lengths_s[s]
        query_at = lax.broadcasted_iota(jnp.int32, (length, length), 0)
        key_at = lax.broadcasted_iota(jnp.int32, (length, length), 1)
        allowed = (key_at <= query_at) & (key_at < here_length)
        for i in range(q_cols // HEAD_SIZE):
            h = j * (q_cols // HEAD_SIZE) + i
            first = h % KEY_VALUE_HEADS * per_head
            blocks = [kv_all[s, first + b] for b in range(per_head)]
            keys = jnp.concatenate([b[:kv_cols] for b in blocks], axis=0)
            values = jnp.concatenate([b[kv_cols:] for b in blocks], axis=0)
            query = qbuf[s, :, pl.ds(h * HEAD_SIZE, HEAD_SIZE)]
            scores = dot(query, keys) * (1.0 / HEAD_SIZE**0.5)
            scores = jnp.where(allowed, scores, jnp.float32(-1e30))
            expo = jnp.exp(scores - jnp.max(scores, axis=1, keepdims=True))
            probs = (expo / jnp.sum(expo, axis=1, keepdims=True)).astype(jnp.bfloat16)
            mixed = dot_nt(probs, values).astype(jnp.bfloat16)
            att_all[j, me_t, rows_of(s), pl.ds(i * HEAD_SIZE, HEAD_SIZE)] = mixed
        for job in att[s][j]:
            job.begin()

    def out_block(s, n):
        rows = pl.ds(pl.multiple_of(s * length, length), length)
        cols = pl.ds(pl.multiple_of(n * o_cols, o_cols), o_cols)
        update = jnp.zeros((length, o_cols), jnp.float32)
        for t in range(tp):
            for j in range(q_steps):
                weight = wo_all[n, t // per_rep, pl.ds(t % per_rep * head_cols + j * q_cols, q_cols), :]
                update = update + dot(att_all[j, t, rows, :], weight)
        block = (raw[rows, cols].astype(jnp.float32) + update).astype(jnp.bfloat16)
        resid[rows, cols] = block
        sums = dot_nt(judge[:, cols], block)
        sums = sums[0:8] + sums[8:16] + sums[16:24]
        line = lax.broadcasted_iota(jnp.int32, sums.shape, 0)
        sums = jnp.where(line == 7, row_sums_of_squares(block), sums)
        stat_here[s] += sums
        return 0

    def project_out(s):
        for job in sum(att[s], wo[:-1]):
            job.need()
        lax.fori_loop(0, o_steps - 1, lambda n, _: out_block(s, n), 0)

    def project_last():
        wo[-1].need()
        lax.fori_loop(0, sequences, lambda s, _: out_block(s, o_steps - 1), 0)

    def judges():
        weight = heads[...] * fgain[...]
        rest = jnp.zeros((8 - heads.shape[0], features), jnp.float32)
        weight = jnp.concatenate([weight, rest], axis=0)
        parts = [p.astype(jnp.float32) for p in exact_parts(weight, 3)]
        stat_here[...] = jnp.zeros_like(stat_here)
        judge[...] = jnp.concatenate(parts + [jnp.zeros_like(weight)], axis=0).astype(jnp.bfloat16)

    def conclude():
        total = stat_all[0]
        for t in range(1, tp):
            total = total + stat_all[t]
        position = lax.broadcasted_iota(jnp.int32, (total.shape[0], length), 1)
        live = [(position < lengths_s[s]).astype(jnp.float32) for s in range(sequences)]
        logits = total * lax.rsqrt(total[7:8] / width + EPS)
        return jnp.where(jnp.concatenate(live, axis=1) > 0.5, logits, jnp.float32(0.0))

    sq.hop(1, DOWN)
    sq.hop(1, UP)
    tok[1][1].begin()
    tok[0][1].hop(1, UP)
    sq.hop(2, DOWN)
    tok[0][1].hop(1, DOWN)
    tok[1][1].hop(1, DOWN)
    tok[0][1].hop(2, DOWN)
    sq.hop(2, UP)
    tok[1][0].begin()
    tok[0][0].turn()
    tok[0][1].hop(2, UP)
    tok[0][0].hop(1, UP)
    tok[0][1].hop(3, DOWN)
    tok[1][1].hop(1, UP)
    tok[0][0].hop(1, DOWN)
    tok[0][1].hop(3, UP)
    tok[0][0].hop(2, UP)
    wq[0].arrive()
    sq.hop(3, DOWN)
    sq.hop(3, UP)
    tok[0][0].hop(3, UP)
    tok[0][0].hop(2, DOWN)
    tok[1][1].hop(2, DOWN)
    tok[0][0].hop(3, DOWN)
    tok[1][1].hop(2, UP)
    judges()
    wkv.arrive()
    tok[1][0].turn()
    project_kv(0)
    tok[1][1].hop(3, DOWN)
    tok[1][1].hop(3, UP)
    tok[1][0].hop(1, UP)
    kv[0].hop(1, UP)
    kv[0].hop(1, DOWN)
    project_q(0, 0)
    tok[1][0].hop(1, DOWN)
    wq[1].arrive()
    kv[0].hop(2, UP)
    tok[1][0].hop(2, UP)
    kv[0].hop(2, DOWN)
    tok[1][0].hop(2, DOWN)
    kv[0].hop(3, DOWN)
    kv[0].hop(3, UP)
    project_q(0, 1)
    tok[1][0].hop(3, UP)
    tok[1][0].hop(3, DOWN)
    project_kv(1)
    attend(0, 1)
    attend(0, 0)
    kv[1].hop(1, DOWN)
    kv[1].hop(1, UP)
    project_q(1, 0)
    att[0][1][0].turn()
    att[0][1][1].hop(1, UP)
    kv[1].hop(2, UP)
    att[0][0][0].turn()
    att[0][1][1].hop(1, DOWN)
    kv[1].hop(2, DOWN)
    att[0][0][1].hop(1, UP)
    kv[1].hop(3, UP)
    att[0][0][1].hop(1, DOWN)
    project_q(1, 1)
    kv[1].hop(3, DOWN)
    att[0][1][1].hop(2, DOWN)
    att[0][1][1].hop(2, UP)
    att[0][0][1].hop(2, UP)
    att[0][0][1].hop(2, DOWN)
    attend(1, 1)
    att[0][1][0].hop(1, DOWN)
    att[0][0][0].hop(1, UP)
    att[0][1][0].hop(1, UP)
    att[0][1][1].hop(3, DOWN)
    attend(1, 0)
    att[1][1][1].hop(1, DOWN)
    att[1][1][1].hop(1, UP)
    att[1][1][0].turn()
    att[1][0][1].hop(1, DOWN)
    wo[0].arrive()
    att[0][1][0].hop(2, UP)
    att[1][0][1].hop(1, UP)
    att[1][1][1].hop(2, UP)
    att[1][0][0].turn()
    att[0][0][0].hop(2, UP)
    att[0][1][1].hop(3, UP)
    att[1][1][1].hop(2, DOWN)
    att[1][0][1].hop(2, UP)
    att[0][0][0].hop(1, DOWN)
    att[1][0][1].hop(2, DOWN)
    att[0][0][1].hop(3, UP)
    att[1][0][0].hop(1, DOWN)
    wo[1].arrive()
    att[0][1][0].hop(2, DOWN)
    wo[2].arrive()
    att[1][1][0].hop(1, UP)
    att[0][0][1].hop(3, DOWN)
    att[1][1][1].hop(3, UP)
    att[1][1][0].hop(1, DOWN)
    att[1][0][0].hop(1, UP)
    att[1][1][1].hop(3, DOWN)
    att[0][0][0].hop(3, UP)
    att[1][0][1].hop(3, UP)
    att[0][1][0].hop(3, UP)
    att[1][0][1].hop(3, DOWN)
    att[0][0][0].hop(2, DOWN)
    att[1][1][0].hop(2, DOWN)
    att[1][0][0].hop(2, UP)
    att[0][0][0].hop(3, DOWN)
    att[1][1][0].hop(2, UP)
    att[1][0][0].hop(3, UP)
    att[0][1][0].hop(3, DOWN)
    project_out(0)
    att[1][1][0].hop(3, UP)
    att[1][1][0].hop(3, DOWN)
    att[1][0][0].hop(2, DOWN)
    att[1][0][0].hop(3, DOWN)
    wo[3].arrive()
    project_out(1)
    project_last()
    stat_all[me_t] = jnp.concatenate([stat_here[s] for s in range(sequences)], axis=1)
    stat.begin()
    writes = [fetch(resid, resid_h)]
    for job in sum(tok + sum(att, []), []) + kv + [sq, wkv] + wq + wo:
        job.drain()
    stat.gathered()
    score[...] = conclude()[: score.shape[0]]
    writes.append(fetch(score, score_h))
    stat.drain()
    for copy in writes:
        copy.wait()


def pass_on_kernel(pieces, resid_in, score_in, resid_out, score_out, resid, score, sems):
    rows = resid.shape[0] // pieces
    parts = [slice(i * rows, (i + 1) * rows) for i in range(pieces)]
    sources = [score_in] + [resid_in.at[p] for p in parts]
    places = [score] + [resid.at[p] for p in parts]
    targets = [score_out] + [resid_out.at[p] for p in parts]
    into = [
        pltpu.make_async_copy(a, b, sems.at[0, i]) for i, (a, b) in enumerate(zip(sources, places))
    ]
    out = [
        pltpu.make_async_copy(a, b, sems.at[1, i]) for i, (a, b) in enumerate(zip(places, targets))
    ]
    for copy in into:
        copy.start()
    for first, second in zip(into, out):
        first.wait()
        second.start()
    for copy in out:
        copy.wait()


def hand_over(resid, score):
    pieces = 4
    anywhere = pl.BlockSpec(memory_space=pl.ANY)
    return pl.pallas_call(
        functools.partial(pass_on_kernel, pieces),
        out_shape=tuple(jax.ShapeDtypeStruct(a.shape, a.dtype) for a in (resid, score)),
        in_specs=[anywhere] * 2,
        out_specs=(anywhere,) * 2,
        scratch_shapes=[
            pltpu.VMEM(resid.shape, resid.dtype),
            pltpu.VMEM(score.shape, score.dtype),
            pltpu.SemaphoreType.DMA((2, pieces + 1)),
        ],
    )(resid, score)


def whole_layer(
    sizes,
    tokens,
    row_lengths,
    attn_gain,
    query_weight,
    key_weight,
    value_matrix,
    output_weight,
    final_gain,
    value_head,
):
    tp, rep = sizes["tp"], sizes["rep"]
    rows, features = tokens.shape
    sequences = row_lengths.shape[0]
    length = rows // sequences
    depth, head_cols = query_weight.shape
    kv_cols = key_weight.shape[1]
    mixed = output_weight.shape[0]
    vmem, dma = pltpu.VMEM, pltpu.SemaphoreType.DMA
    half, single = jnp.bfloat16, jnp.float32
    q_steps, o_steps = head_cols // STEP, features // STEP
    anywhere = pl.BlockSpec(memory_space=pl.ANY)
    resid, score = pl.pallas_call(
        functools.partial(layer_kernel, sizes),
        out_shape=(
            jax.ShapeDtypeStruct((rows, features), half),
            jax.ShapeDtypeStruct((value_head.shape[1], rows), single),
        ),
        in_specs=[pl.BlockSpec(memory_space=pltpu.SMEM)] + [pl.BlockSpec(memory_space=pltpu.HBM)] * 8,
        out_specs=(anywhere, anywhere),
        scratch_shapes=[
            vmem((tp, rows, features), half),
            vmem((rep, 2 * kv_cols, depth), half),
            vmem((q_steps, rep, depth, STEP), half),
            vmem((o_steps, rep, mixed, STEP), half),
            vmem((sequences, tp, 2 * kv_cols, length), half),
            vmem((q_steps, tp, rows, STEP), half),
            vmem((tp, 8, rows), single),
            vmem((tp, 8, rows), single),
            vmem((sequences, 8, length), single),
            vmem((rows, features), half),
            vmem((1, features), single),
            vmem((1, features), single),
            vmem((value_head.shape[1], features), single),
            vmem((32, features), half),
            vmem((sequences, length, head_cols), half),
            vmem((rows, features), half),
            vmem((value_head.shape[1], rows), single),
            dma((SEMAPHORES,)),
            dma((16,)),
        ],
        compiler_params=pltpu.CompilerParams(
            collective_id=4, has_side_effects=True, vmem_limit_bytes=64 * 1024 * 1024 - 128 * 1024
        ),
    )(
        row_lengths,
        tokens,
        attn_gain[None, :],
        query_weight,
        key_weight.T,
        value_matrix.T,
        output_weight,
        final_gain[None, :],
        value_head.T,
    )
    resid, score = hand_over(resid, score)
    return resid, score.T


def fits(sizes, tokens, row_lengths, query_weight, key_weight):
    heads = query_weight.shape[1] // HEAD_SIZE
    return (
        row_lengths.shape[0] == 2
        and sizes["rep"] == 4
        and sizes["tp"] % sizes["rep"] == 0
        and sizes["tp"] == 8
        and heads > 0
        and heads % KEY_VALUE_HEADS == 0
        and query_weight.shape[1] == 2 * STEP
        and tokens.shape[1] == 4 * STEP
        and HEAD_SIZE % key_weight.shape[1] == 0
    )


def layer(sizes, tokens, row_lengths, attn_gain, query_weight, key_weight, *rest):
    chosen = whole_layer if fits(sizes, tokens, row_lengths, query_weight, key_weight) else local
    return chosen(sizes, tokens, row_lengths, attn_gain, query_weight, key_weight, *rest)


def solution(mesh):
    in_specs = (
        P("rep", "tp"),
        P("rep"),
        P("tp"),
        P("rep", "tp"),
        P("rep", "tp"),
        P("rep", "tp"),
        P("rep", "tp"),
        P("tp"),
        P("tp", None),
    )
    out_specs = (P("rep", "tp"), P("rep", None))
    body = functools.partial(layer, dict(mesh.shape))
    return jax.shard_map(body, mesh=mesh, in_specs=in_specs, out_specs=out_specs, check_vma=False)
```
